32 devices in a mesh: cells: 16 (over z, y, x), faces: 2 (over core).
Axes of the slice: x: 2, y: 2, z: 4, core: 2. Of those that a mesh axis runs over, the one named last changes fastest.
Arguments:
- flow_state: float32 [4, 131072], P(None, 'cells'), may hold values from -6 to 6
- source_term: float32 [4, 131072], P(None, 'cells'), may hold values from -24 to 24
- volume_rate: float32 [131072], P('cells'), may hold values from 0.5 to 4
- face_normal: float32 [3, 393216], P(None, ('cells', 'faces')), may hold values from -3 to 3
- face_owner: int32 [393216], P(('cells', 'faces')), may hold values from 0 to 8191, as said below
- face_neighbour: int32 [393216], P(('cells', 'faces')), may hold values from 0 to 9727, as said below
- face_count: int32 [32], P(('cells', 'faces')), may hold values from 1536 to 12288, as said below
- send_list: int32 [96, 256], P('cells'), may hold values from 0 to 8191
- halo_count: int32 [96], P('cells'), may hold values from 64 to 256, as said below
Outputs:
- solution_field: float32 [4, 131072], P(None, 'cells')
- residual: float32 [4, 131072], P(None, 'cells')
The draws below stay inside these ranges and needn't reach their ends.
Inputs may be any that keep to these rules, and one draw needn't show every extreme that they name: `face_owner`: A local cell of the slot's partition; with s = g mod 12288 and t = s // 192, it lies in 128 * t to 128 * t + 127. `face_neighbour`: with s and t as for face_owner: below 8192 a local cell (128 * t + d) mod 8192 with d in 0 to 255; otherwise 8192 plus a halo slot of the slot's partition in (t mod (6)) * 256 to that plus 256 - 1. Live slots of a block are its first face_count slots; in every draw some block has all 12288 slots live. `send_list`: entries at or past the list's count are unused. `halo_count`: every partition has one list with exactly 256 entries.
All inputs are finite; a program needn't handle non-finite values.
Results may differ from the reference program's by a relative error of at most 0.0003.
Values sent between devices are 32-bit elements; how exact they have to be, the bound alone decides.
A program may use at most 64 MiB of HBM per device.

```python
import math
import jax
import jax.numpy as jnp
from jax import lax

CELLS_DEV = 8192
HALO = 256
NEIGH = 3
ITERS = 2
BLOCK = 4
TILES = 64
HWIN = 256
PARTITIONS = 16
SPLIT = 2
GROUPS = 32
FACE_SLOTS = 12288
CELLS = 131072
FACES = 393216


def draw_face_count(key, part):
    drawn_counts = jax.random.randint(key, (GROUPS,), FACE_SLOTS // 8, FACE_SLOTS + 1)
    chosen = jax.random.randint(jax.random.fold_in(key, 7), (), 0, GROUPS)
    return jnp.where(jnp.arange(GROUPS) == chosen, FACE_SLOTS, drawn_counts).astype(jnp.int32)


def draw_halo_count(key, part):
    list_total = 2 * NEIGH
    drawn_counts = jax.random.randint(key, (PARTITIONS, list_total), HALO // 4, HALO + 1)
    chosen = jax.random.randint(jax.random.fold_in(key, 11), (PARTITIONS, 1), 0, list_total)
    filled = jnp.where(jnp.arange(list_total)[None, :] == chosen, HALO, drawn_counts)
    return filled.reshape(PARTITIONS * list_total).astype(jnp.int32)


def tile_of_slot():
    slot_ids = jnp.arange(FACES, dtype=jnp.int32) % FACE_SLOTS
    return slot_ids // (FACE_SLOTS // TILES)


def draw_face_owner(key, part):
    tile_ids = tile_of_slot()
    offset = jax.random.randint(jax.random.fold_in(key, 21), (FACES,), 0, 128)
    return (tile_ids * 128 + offset).astype(jnp.int32)


def draw_face_neighbour(key, part):
    tile_ids = tile_of_slot()
    window_count = 2 * NEIGH * HALO // HWIN
    local_offset = jax.random.randint(jax.random.fold_in(key, 31), (FACES,), 0, 256)
    local_cell = (tile_ids * 128 + local_offset) % CELLS_DEV
    halo_offset = jax.random.randint(jax.random.fold_in(key, 37), (FACES,), 0, HWIN)
    halo_cell = CELLS_DEV + tile_ids % window_count * HWIN + halo_offset
    pick = jax.random.randint(jax.random.fold_in(key, 41), (FACES,), 0, 10)
    return jnp.where(pick < 3, halo_cell, local_cell).astype(jnp.int32)


def with_ends(values, key, least, high):
    place = [jax.random.randint(jax.random.fold_in(key, axis), (), 0, length) for axis, length in enumerate(values.shape)]
    main_axis = values.shape.index(max(values.shape))
    next_to = place[:main_axis] + [(place[main_axis] + 1) % values.shape[main_axis]] + place[main_axis + 1:]
    return values.at[tuple(place)].set(least).at[tuple(next_to)].set(high)


def shard_levels(stream_key, shape, shards, low, largest):
    loudness = 1.0
    for position, shards_of in shards:
        heights = jax.random.uniform(jax.random.fold_in(jax.random.fold_in(stream_key, 6), position), (shards_of,), jnp.float32, low / len(shards), largest / len(shards))
        loudness = loudness * jnp.repeat(jnp.exp(heights), shape[position] // shards_of).reshape((-1,) + (1,) * (len(shape) - 1 - position))
    return loudness


def bell_draw(stream_key, extent, width, limit, shards=(), kind=jnp.bfloat16):
    drawn = jax.random.normal(stream_key, extent, jnp.float32) * width
    if len(shards) > 0:
        drawn = shard_levels(stream_key, extent, shards, -0.22, 0.18) * drawn
    return jnp.clip(drawn, min=-limit, max=limit).astype(kind)


def setup_inputs(seed: int = 0) -> dict:
    key_list = jax.random.split(jax.random.key(seed), 10)
    return {
        "flow_state": bell_draw(key_list[0], (BLOCK, CELLS), 1.0, 6.0, ((1, 16),), jnp.float32),
        "source_term": bell_draw(key_list[1], (BLOCK, CELLS), 4.0, 24.0, ((1, 16),), jnp.float32),
        "volume_rate": jnp.clip(jnp.exp(math.log(4.0) - 2.0794415 * jax.random.uniform(key_list[2], (CELLS,), jnp.float32) ** shard_levels(key_list[2], (CELLS,), ((0, 16),), -0.2, 0.2)), 0.5, 4.0),
        "face_normal": bell_draw(key_list[3], (3, FACES), 0.5, 3.0, ((1, 32),), jnp.float32),
        "face_owner": draw_face_owner(jax.random.fold_in(key_list[9], 71), 0),
        "face_neighbour": draw_face_neighbour(jax.random.fold_in(key_list[9], 71), 0),
        "face_count": draw_face_count(jax.random.fold_in(key_list[9], 71), 0),
        "send_list": with_ends(jax.random.randint(key_list[7], (PARTITIONS * 2 * NEIGH, HALO), 0, CELLS_DEV), jax.random.fold_in(key_list[7], 1), 0, CELLS_DEV - 1).astype(jnp.int32),
        "halo_count": draw_halo_count(jax.random.fold_in(key_list[9], 71), 0),
    }


def shift_table():
    return jnp.array([which + 1 for which in range(NEIGH)] + [-(which + 1) for which in range(NEIGH)], jnp.int32)

def reference(flow_state, source_term, volume_rate, face_normal, face_owner, face_neighbour, face_count, send_list, halo_count):
    list_total = 2 * NEIGH
    face_ids = jnp.arange(FACES, dtype=jnp.int32)
    partition = face_ids // (FACE_SLOTS * SPLIT)
    is_live = (face_ids % FACE_SLOTS < face_count[face_ids // FACE_SLOTS]).astype(jnp.float32)
    owner_global = partition * CELLS_DEV + face_owner
    is_local = face_neighbour < CELLS_DEV
    halo_pos = jnp.maximum(face_neighbour - CELLS_DEV, 0)
    which_list = halo_pos // HALO
    which_slot = halo_pos % HALO
    sender = (partition - shift_table()[which_list]) % PARTITIONS
    list_row = sender * list_total + which_list
    sent_cell = send_list[list_row, which_slot]
    halo_live = which_slot < halo_count[list_row]
    neighbour_global = jnp.where(is_local, partition * CELLS_DEV + face_neighbour, sender * CELLS_DEV + sent_cell)
    neighbour_weight = jnp.where(is_local | halo_live, 1.0, 0.0).astype(jnp.float32)
    local_weight = is_local.astype(jnp.float32)
    sink_index = jnp.where(is_local, neighbour_global, CELLS)
    index_both = jnp.concatenate([owner_global, sink_index])

    def to_cells(owner_values, neighbour_values):
        stacked = jnp.concatenate([owner_values, neighbour_values], axis=1).T
        summed = jax.ops.segment_sum(stacked, index_both, num_segments=CELLS + 1)
        return summed[:CELLS].T
    left_state = flow_state[:, owner_global]
    right_state = flow_state[:, neighbour_global] * neighbour_weight
    normal_speed = 0.5 * lax.optimization_barrier(jnp.sum(face_normal * (left_state[:3] + right_state[:3]), axis=0))
    normal_size = jnp.sqrt(lax.optimization_barrier(jnp.sum(face_normal * face_normal, axis=0)))
    wave_speed = jnp.abs(normal_speed) + 2.0 * normal_size
    owner_terms = 0.5 * jnp.concatenate([normal_speed[None], face_normal, wave_speed[None]], axis=0) * is_live
    neighbour_terms = jnp.concatenate([-0.5 * normal_speed[None], -0.5 * face_normal, 0.5 * wave_speed[None]], axis=0) * (is_live * local_weight)
    block_terms = to_cells(owner_terms, neighbour_terms)
    velocity_diag = volume_rate + block_terms[0] + block_terms[4]
    pressure_diag = volume_rate + block_terms[4]
    coupling = block_terms[1:4]
    schur = pressure_diag - lax.optimization_barrier(jnp.sum(coupling * coupling, axis=0)) / velocity_diag

    def precondition(vector_in):
        pressure = (vector_in[3] - lax.optimization_barrier(jnp.sum(coupling * vector_in[:3], axis=0)) / velocity_diag) / schur
        velocity = (vector_in[:3] - coupling * pressure) / velocity_diag
        return jnp.concatenate([velocity, pressure[None]], axis=0)

    def apply_matrix(vector_in):
        left_side = vector_in[:, owner_global]
        right_side = vector_in[:, neighbour_global] * neighbour_weight
        face_sum = left_side + right_side
        central = jnp.concatenate([normal_speed * face_sum[:3] + face_normal * face_sum[3], lax.optimization_barrier(jnp.sum(face_normal * face_sum[:3], axis=0))[None]], axis=0)
        face_flux = (0.5 * central - 0.5 * wave_speed * (right_side - left_side)) * is_live
        return volume_rate * vector_in + to_cells(face_flux, -face_flux * local_weight)
    solution_field = jnp.zeros_like(source_term)
    residual = source_term
    shadow = source_term
    direction = source_term
    rho_now = jnp.sum(shadow * residual)
    for iteration in range(ITERS):
        pre_dir = precondition(direction)
        image = apply_matrix(pre_dir)
        step_alpha = rho_now / jnp.sum(shadow * image)
        middle = residual - step_alpha * image
        pre_mid = precondition(middle)
        second = apply_matrix(pre_mid)
        step_omega = jnp.sum(second * middle) / jnp.sum(second * second)
        solution_field = solution_field + step_alpha * pre_dir + step_omega * pre_mid
        residual = middle - step_omega * second
        if iteration + 1 < ITERS:
            rho_next = jnp.sum(shadow * residual)
            ratio_beta = rho_next / rho_now * (step_alpha / step_omega)
            direction = residual + ratio_beta * (direction - step_omega * image)
            rho_now = rho_next
    return (solution_field, residual)
```

```python
import functools

import jax
import jax.numpy as jnp
from jax import lax
from jax.experimental import pallas as pl
from jax.experimental.pallas import tpu as pltpu
from jax.sharding import PartitionSpec as P

ITERS = 2
LANES = 128
MESH = pl.DeviceIdType.MESH
F32 = jnp.float32
BF16 = jnp.bfloat16


def take_lanes(source, index):
    return jnp.take_along_axis(source, index, axis=1, mode="promise_in_bounds")


def split(value):
    high = value.astype(BF16).astype(F32)
    return high, value - high


def kernel(
    parts,
    cores,
    count_ref,
    flow_hbm,
    source_hbm,
    volume_hbm,
    normal_hbm,
    owner_hbm,
    neighbour_hbm,
    list_ref,
    halo_count_ref,
    solution_ref,
    residual_ref,
    flow_ref,
    source_ref,
    volume_ref,
    normal_ref,
    owner_ref,
    neighbour_ref,
    input_sem,
    own_lane,
    right_lane,
    right_kind,
    own_row,
    local_row,
    face_u,
    face_s,
    face_n,
    signed_hot,
    plain_hot,
    flux_rows,
    size_rows,
    cell_rows,
    size_cells,
    fields,
    halo_rows,
    blocks,
    vecs,
    pair_out,
    pair_in,
    halo_out,
    halo_in,
    dot_out,
    dot_in,
    pair_send,
    pair_recv,
    halo_send,
    halo_recv,
    dot_send,
    dot_recv,
):
    me = lax.axis_index("cells")
    core = lax.axis_index("faces")
    other = (core + 1) % cores
    tiles = volume_ref.shape[0]
    pairs = tiles // 2
    groups = pairs // 8
    cells = tiles * LANES
    lists = halo_in.shape[1]
    lists_here = lists // cores
    width = list_ref.shape[1] * LANES

    def fetched(number, source, target):
        copy = pltpu.make_async_copy(source, target, input_sem.at[number])
        copy.start()
        return copy

    copies = [
        fetched(0, owner_hbm, owner_ref),
        fetched(1, neighbour_hbm, neighbour_ref),
        fetched(2, flow_hbm, flow_ref),
        fetched(4, source_hbm, source_ref),
        fetched(5, volume_hbm, volume_ref),
    ]
    normals = [fetched(3, normal_hbm, normal_ref.at[pl.ds(0, 3 * pairs)])]

    barrier = pltpu.get_barrier_semaphore()
    for step in range(1, parts * cores):
        number = (me * cores + core + step) % (parts * cores)
        pl.semaphore_signal(
            barrier,
            inc=1,
            device_id={"cells": number // cores, "faces": number % cores},
            device_id_type=MESH,
        )

    lane = lax.broadcasted_iota(jnp.int32, (pairs, LANES), 1)
    pair_id = lax.broadcasted_iota(jnp.int32, (pairs, LANES), 0)
    late = lane >= LANES // 2
    count = count_ref[0]
    for copy in copies:
        copy.wait()
    for j in range(3):
        tile = 2 * pair_id + (0 if j == 0 else 1)
        if j == 1:
            tile = 2 * pair_id + late.astype(jnp.int32)
        owner = owner_ref[pl.ds(j, pairs, stride=3), :]
        beside = neighbour_ref[pl.ds(j, pairs, stride=3), :]
        live = (3 * pair_id + j) * LANES + lane < count
        is_local = beside < cells
        column = beside - tile * LANES
        column = jnp.where(column < 0, column + cells, column)
        slot = beside - cells - (tile % lists) * width
        place = jnp.where(is_local, column, slot)
        upper = place >= LANES
        own = owner - tile * LANES
        own_lane[j] = own
        right_lane[j] = jnp.where(upper, place - LANES, place)
        right_kind[j] = jnp.where(is_local, 0, 2) + upper.astype(jnp.int32)
        own_row[j] = jnp.where(live, own, -1).astype(F32)
        local_row[j] = jnp.where(live & is_local, column, -1).astype(F32)

    def start_halo(turn, field):
        row8 = lax.broadcasted_iota(jnp.int32, (8, LANES), 0)
        for i in range(lists_here):
            which = core * lists_here + i
            rows = []
            wanted = list_ref[which]
            limit = halo_count_ref[which]
            for b in range(4):
                for half in range(2):
                    cell = jnp.broadcast_to(wanted[half : half + 1], (8, LANES))
                    row = cell // LANES
                    col = cell - row * LANES
                    found = jnp.zeros((8, LANES), F32)
                    for g in range(tiles // 8):
                        got = take_lanes(field(b, g), col)
                        found = jnp.where(row == row8 + 8 * g, got, found)
                    found = jnp.sum(found, axis=0, keepdims=True)
                    used = (
                        lax.broadcasted_iota(jnp.int32, (1, LANES), 1) + half * LANES < limit
                    )
                    rows.append(jnp.where(used, found, 0.0))
            halo_out[turn, i] = jnp.concatenate(rows, axis=0)
        for i in range(lists_here):
            target = (me + (1 - 2 * core) * (i + 1) + parts) % parts
            for c in range(cores):
                pltpu.make_async_remote_copy(
                    src_ref=halo_out.at[turn, i],
                    dst_ref=halo_in.at[turn, core * lists_here + i],
                    send_sem=halo_send.at[turn],
                    recv_sem=halo_recv.at[turn],
                    device_id={"cells": target, "faces": c},
                    device_id_type=MESH,
                ).start()

    def wait_halo(turn):
        pltpu.make_async_copy(halo_in.at[turn], halo_in.at[turn], halo_recv.at[turn]).wait()
        return [halo_in[turn, k] for k in range(lists)]

    def start_pair(turn, rows):
        copy = pltpu.make_async_remote_copy(
            src_ref=pair_out.at[turn, pl.ds(0, rows)],
            dst_ref=pair_in.at[turn, pl.ds(0, rows)],
            send_sem=pair_send.at[turn],
            recv_sem=pair_recv.at[turn],
            device_id={"cells": me, "faces": other},
            device_id_type=MESH,
        )
        copy.start()
        return copy

    def start_dots(turn, partials):
        at = lax.broadcasted_iota(jnp.int32, (1, LANES), 1)
        packed = jnp.zeros((1, LANES), F32)
        for d, p in enumerate(partials):
            row = jnp.sum(p.reshape(tiles // 8, 8, LANES).sum(axis=0), axis=0, keepdims=True)
            packed = jnp.where(at == d, jnp.sum(row, axis=1, keepdims=True), packed)
        dot_out[turn] = packed
        dot_in[turn, me] = packed
        for step in range(1, parts):
            pltpu.make_async_remote_copy(
                src_ref=dot_out.at[turn],
                dst_ref=dot_in.at[turn, me],
                send_sem=dot_send.at[turn],
                recv_sem=dot_recv.at[turn],
                device_id={"cells": (me + step) % parts, "faces": core},
                device_id_type=MESH,
            ).start()

    def wait_dots(turn, number):
        part = dot_in.at[turn, pl.ds(0, parts - 1)]
        pltpu.make_async_copy(part, part, dot_recv.at[turn]).wait()
        total = dot_in[turn, 0]
        for q in range(1, parts):
            total = total + dot_in[turn, q]
        return [jnp.broadcast_to(total[:, d : d + 1], (1, LANES)) for d in range(number)]

    def put_field(values, halos):
        for b, value in enumerate(values):
            fields[b, pl.ds(0, tiles), :] = value
            fields[b, pl.ds(tiles, 1), :] = value[0:1]
        period = halo_rows.shape[0] // 8
        for t in range(period):
            halo_rows[pl.ds(t, 8, stride=period), :] = halos[t % lists]

    def sides(g, j, b):
        period = halo_rows.shape[0] // 8
        here = pl.multiple_of(g * 8, 8)
        left_at = own_lane[j, pl.ds(here, 8), :]
        right_at = right_lane[j, pl.ds(here, 8), :]
        kind = right_kind[j, pl.ds(here, 8), :]

        def of_tile(odd):
            first = 16 * g + odd
            halo_first = (16 * g) % lists + odd
            low = fields[b, pl.ds(first, 8, stride=2), :]
            high = fields[b, pl.ds(first + 1, 8, stride=2), :]
            halo_low = halo_rows[pl.ds(2 * b * period + halo_first, 8, stride=2), :]
            halo_high = halo_rows[pl.ds((2 * b + 1) * period + halo_first, 8, stride=2), :]
            left = take_lanes(low, left_at)
            right = jnp.where(
                kind < 2,
                jnp.where(kind == 0, take_lanes(low, right_at), take_lanes(high, right_at)),
                jnp.where(
                    kind == 2, take_lanes(halo_low, right_at), take_lanes(halo_high, right_at)
                ),
            )
            return left, right

        if j == 0:
            return of_tile(0)
        if j == 2:
            return of_tile(1)
        early = lax.broadcasted_iota(jnp.int32, (8, LANES), 1) < LANES // 2
        left_a, right_a = of_tile(0)
        left_b, right_b = of_tile(1)
        return jnp.where(early, left_a, left_b), jnp.where(early, right_a, right_b)

    def put_flux(ref, g, j, b, value):
        high, low = split(value)
        ref[j, pl.ds(64 * g + b, 8, stride=8), :] = high
        ref[j, pl.ds(64 * g + 4 + b, 8, stride=8), :] = low

    def tile_rows(rows_ref, u, odd):
        at = pl.ds(pl.multiple_of(u * 8, 8), 8)
        middle = rows_ref[1, at, :]
        if odd:
            middle = pltpu.roll(middle, LANES // 2, 1)
        rows = jnp.concatenate([rows_ref[2 * odd, at, :], middle], axis=1)
        return rows[:, : 3 * LANES // 2]

    def added(rows, hot):
        return lax.dot_general(
            rows.astype(BF16), hot, (((1,), (0,)), ((), ())), preferred_element_type=F32
        )

    def scatter(u):
        for odd in range(2):
            result = added(tile_rows(flux_rows, u, odd), signed_hot[2 * u + odd])
            at = pl.ds(pl.multiple_of(u * 16 + odd * 8, 8), 8)
            cell_rows[0, at, :] = result[:, :LANES]
            cell_rows[1, at, :] = result[:, LANES:]

    def scatter_size(u):
        for odd in range(2):
            sizes = tile_rows(size_rows, u, odd)
            rows = jnp.concatenate([tile_rows(flux_rows, u, odd), sizes], axis=0)
            at = pl.ds(pl.multiple_of(u * 16 + odd * 8, 8), 8)
            result = added(rows, signed_hot[2 * u + odd])
            cell_rows[0, at, :] = result[:8, :LANES]
            cell_rows[1, at, :] = result[:8, LANES:]
            size_cells[0, at, :] = added(sizes, plain_hot[2 * u + odd])
            size_cells[1, at, :] = -result[8:, LANES:]

    def collect(cells_ref, b):
        def rows(first, side):
            return cells_ref[side, pl.ds(first, tiles, stride=8), :]

        low = rows(b, 0) + rows(4 + b, 0)
        high = rows(b, 1) + rows(4 + b, 1)
        high = jnp.concatenate([high[tiles - 1 :], high[: tiles - 1]], axis=0)
        return low + high

    def apply_matrix(turn, values, halos):
        put_field(values, halos)

        def group(g, carry):
            here = pl.multiple_of(g * 8, 8)
            for j in range(3):
                u = face_u[j, pl.ds(here, 8), :]
                s = face_s[j, pl.ds(here, 8), :]
                n = [face_n[i, j, pl.ds(here, 8), :] for i in range(3)]
                both = [sides(g, j, b) for b in range(4)]
                total = [left + right for left, right in both]
                jump = [s * (right - left) for left, right in both]
                for i in range(3):
                    put_flux(flux_rows, g, j, i, u * total[i] + n[i] * total[3] - jump[i])
                last = n[0] * total[0] + n[1] * total[1] + n[2] * total[2] - jump[3]
                put_flux(flux_rows, g, j, 3, last)
            for i in range(8):
                scatter(g * 8 + i)
            return carry

        lax.fori_loop(0, groups, group, 0)
        mine = [collect(cell_rows, b) for b in range(4)]
        for b in range(4):
            pair_out[turn, b * tiles : (b + 1) * tiles, :] = mine[b]
        copy = start_pair(turn, 4 * tiles)
        copy.wait_recv()
        volume = volume_ref[...]
        return [
            volume * values[b]
            + (
                pair_out[turn, b * tiles : (b + 1) * tiles, :]
                + pair_in[turn, b * tiles : (b + 1) * tiles, :]
            )
            for b in range(4)
        ]

    def precondition(w):
        rvd, rschur = blocks[0], blocks[1]
        n = [blocks[2 + i] for i in range(3)]
        pressure = (w[3] - (n[0] * w[0] + n[1] * w[1] + n[2] * w[2]) * rvd) * rschur
        return [(w[i] - n[i] * pressure) * rvd for i in range(3)] + [pressure]

    def load(which):
        return [vecs[which, b] for b in range(4)]

    def save(which, values):
        for b in range(4):
            vecs[which, b] = values[b]

    def dot(a, b):
        return a[0] * b[0] + a[1] * b[1] + a[2] * b[2] + a[3] * b[3]

    def saved_field(which):
        return lambda b, g: vecs[which, b, 8 * g : 8 * g + 8, :]

    PRE, IMAGE_M, TEMP = 0, 1, 2
    flow = [flow_ref[pl.ds(b, tiles, stride=4), :] for b in range(4)]
    source = [source_ref[pl.ds(b, tiles, stride=4), :] for b in range(4)]
    pl.semaphore_wait(barrier, parts * cores - 1)
    start_halo(0, lambda b, g: flow_ref[pl.ds(32 * g + b, 8, stride=4), :])
    start_dots(0, [dot(source, source)])

    cell_id = lax.broadcasted_iota(jnp.int32, (LANES, LANES), 1).astype(F32).astype(BF16)
    one, zero = jnp.ones((), BF16), jnp.zeros((), BF16)

    def by_face(rows):
        flat = rows[...].reshape(3 * pairs, LANES)
        spare = -(3 * pairs) % LANES
        flat = jnp.concatenate([flat, jnp.zeros((spare, LANES), F32)], axis=0)
        return flat.T.astype(BF16)

    own_faces, local_faces = by_face(own_row), by_face(local_row)

    def hot_of(column):
        return jnp.where(cell_id == column, one, zero)

    for u in range(pairs):
        for j in range(3):
            at = j * pairs + u
            own = jnp.broadcast_to(own_faces[:, at : at + 1], (LANES, LANES))
            local = jnp.broadcast_to(local_faces[:, at : at + 1], (LANES, LANES))
            own_hot, local_hot = hot_of(own), hot_of(local)
            low = own_hot - local_hot
            high = -hot_of(local - LANES)
            plain = own_hot + local_hot
            half = LANES // 2
            if j == 1:
                places = [(2 * u, LANES, 0, half), (2 * u + 1, LANES, half, LANES)]
            else:
                places = [(2 * u + j // 2, 0, 0, LANES)]
            for tile, row, first, last in places:
                rows = slice(row, row + last - first)
                signed_hot[tile, rows, :LANES] = low[first:last]
                signed_hot[tile, rows, LANES:] = high[first:last]
                plain_hot[tile, rows, :] = plain[first:last]

    size_rows[...] = jnp.zeros_like(size_rows)
    for copy in normals:
        copy.wait()

    put_field(flow, wait_halo(0))

    def face_terms(g, carry):
        here = pl.multiple_of(g * 8, 8)
        for j in range(3):
            n = [normal_ref[pl.ds(24 * g + j, 8, stride=3), i, :] for i in range(3)]
            both = [sides(g, j, b) for b in range(3)]
            total = [left + right for left, right in both]
            u = 0.5 * (n[0] * total[0] + n[1] * total[1] + n[2] * total[2])
            s = jnp.abs(u) + 2.0 * jnp.sqrt(n[0] * n[0] + n[1] * n[1] + n[2] * n[2])
            u, s = 0.5 * u, 0.5 * s
            n = [0.5 * n[i] for i in range(3)]
            face_u[j, pl.ds(here, 8), :] = u
            face_s[j, pl.ds(here, 8), :] = s
            put_flux(flux_rows, g, j, 0, u)
            for i in range(3):
                face_n[i, j, pl.ds(here, 8), :] = n[i]
                put_flux(flux_rows, g, j, 1 + i, n[i])
            put_flux(size_rows, g, j, 0, s)
        for i in range(8):
            scatter_size(g * 8 + i)
        return carry

    lax.fori_loop(0, groups, face_terms, 0)
    for b in range(4):
        pair_out[0, b * tiles : (b + 1) * tiles, :] = collect(cell_rows, b)
    pair_out[0, 4 * tiles : 5 * tiles, :] = collect(size_cells, 0)
    start_pair(0, 5 * tiles).wait_recv()
    sums = [
        pair_out[0, b * tiles : (b + 1) * tiles, :] + pair_in[0, b * tiles : (b + 1) * tiles, :]
        for b in range(5)
    ]
    volume = volume_ref[...]
    rvd = 1.0 / (volume + sums[0] + sums[4])
    coupling = sums[1:4]
    norm = coupling[0] * coupling[0] + coupling[1] * coupling[1] + coupling[2] * coupling[2]
    blocks[0] = rvd
    blocks[1] = 1.0 / (volume + sums[4] - norm * rvd)
    for i in range(3):
        blocks[2 + i] = coupling[i]

    def combine(a, scale, b):
        return [x + scale * y for x, y in zip(a, b)]

    residual = source
    direction = source
    pre_dir = precondition(direction)
    save(PRE, pre_dir)
    start_halo(1, saved_field(PRE))
    (rho,) = wait_dots(0, 1)
    halo_dir = wait_halo(1)
    halo_res = halo_dir
    answer = None
    for iteration in range(ITERS):
        final = iteration + 1 == ITERS
        turn = 1 + 2 * iteration
        image = apply_matrix(turn, pre_dir, halo_dir)
        start_dots(turn, [dot(source, image)])
        pre_image = precondition(image)
        save(IMAGE_M, pre_image)
        start_halo(turn + 1, saved_field(IMAGE_M))
        pre_res = pre_dir if iteration == 0 else precondition(residual)
        (shadow_image,) = wait_dots(turn, 1)
        alpha = rho / shadow_image
        middle = combine(residual, -alpha, image)
        pre_mid = combine(pre_res, -alpha, pre_image)
        halo_image = wait_halo(turn + 1)
        halo_mid = combine(halo_res, -alpha, halo_image)
        second = apply_matrix(turn + 1, pre_mid, halo_mid)
        start_dots(
            turn + 1,
            [dot(second, middle), dot(second, second), dot(source, middle), dot(source, second)],
        )
        if not final:
            pre_second = precondition(second)
            save(TEMP, pre_second)
            start_halo(turn + 2, saved_field(TEMP))
        second_mid, second_sq, shadow_mid, shadow_second = wait_dots(turn + 1, 4)
        omega = second_mid / second_sq
        step = combine([alpha * v for v in pre_dir], omega, pre_mid)
        answer = step if answer is None else [a + s for a, s in zip(answer, step)]
        residual = combine(middle, -omega, second)
        if not final:
            rho_next = shadow_mid - omega * shadow_second
            beta = rho_next / rho * (alpha / omega)
            rho = rho_next
            direction = combine(residual, beta, combine(direction, -omega, image))
            pre_dir = precondition(direction)
            halo_second = wait_halo(turn + 2)
            halo_res = combine(halo_mid, -omega, halo_second)
            halo_dir = combine(halo_res, beta, combine(halo_dir, -omega, halo_image))
    for b in range(4):
        solution_ref[pl.ds(b, tiles, stride=4), :] = answer[b]
        residual_ref[pl.ds(b, tiles, stride=4), :] = residual[b]

    for turn in range(halo_in.shape[0]):
        pltpu.make_async_copy(halo_in.at[turn], halo_in.at[turn], halo_send.at[turn]).wait()
    for turn in range(pair_in.shape[0]):
        part = pair_out.at[turn, pl.ds(0, (5 if turn == 0 else 4) * tiles)]
        pltpu.make_async_copy(part, part, pair_send.at[turn]).wait()
        part = dot_in.at[turn, pl.ds(0, parts - 1)]
        pltpu.make_async_copy(part, part, dot_send.at[turn]).wait()


def body(
    flow_state,
    source_term,
    volume_rate,
    face_normal,
    face_owner,
    face_neighbour,
    face_count,
    send_list,
    halo_count,
):
    parts = lax.axis_size("cells")
    cores = lax.axis_size("faces")
    cells = flow_state.shape[1]
    tiles = cells // LANES
    pairs = tiles // 2
    face_rows = face_owner.shape[0] // LANES
    lists, width = send_list.shape
    period = -(-(lists + 16) // 8) * 8
    turns = 1 + 2 * ITERS

    def by_tile(field):
        return field.reshape(4, tiles, LANES).transpose(1, 0, 2).reshape(4 * tiles, LANES)

    def by_component(field):
        return field.reshape(tiles, 4, LANES).transpose(1, 0, 2).reshape(4, cells)

    vmem = pl.BlockSpec(memory_space=pltpu.VMEM)
    hbm = pl.BlockSpec(memory_space=pl.ANY)
    smem = pl.BlockSpec(memory_space=pltpu.SMEM)
    ints = pltpu.VMEM((3, pairs, LANES), jnp.int32)
    floats = pltpu.VMEM((3, pairs, LANES), F32)
    hot = pltpu.VMEM((tiles, 3 * LANES // 2, 2 * LANES), BF16)
    out = jax.ShapeDtypeStruct((4 * tiles, LANES), F32)
    solved, left = pl.pallas_call(
        functools.partial(kernel, parts, cores),
        out_shape=(out, out),
        in_specs=[smem] + [hbm] * 6 + [vmem, smem],
        out_specs=(vmem, vmem),
        scratch_shapes=[
            pltpu.VMEM((4 * tiles, LANES), F32),
            pltpu.VMEM((4 * tiles, LANES), F32),
            pltpu.VMEM((tiles, LANES), F32),
            pltpu.VMEM((face_rows + 8, 3, LANES), F32),
            pltpu.VMEM((face_rows, LANES), jnp.int32),
            pltpu.VMEM((face_rows, LANES), jnp.int32),
            pltpu.SemaphoreType.DMA((6,)),
            ints,
            ints,
            ints,
            floats,
            floats,
            floats,
            floats,
            pltpu.VMEM((3, 3, pairs, LANES), F32),
            hot,
            pltpu.VMEM((tiles, 3 * LANES // 2, LANES), BF16),
            pltpu.VMEM((3, 8 * pairs, LANES), F32),
            pltpu.VMEM((3, 8 * pairs, LANES), F32),
            pltpu.VMEM((2, 8 * tiles, LANES), F32),
            pltpu.VMEM((2, 8 * tiles, LANES), F32),
            pltpu.VMEM((4, tiles + 8, LANES), F32),
            pltpu.VMEM((8 * period, LANES), F32),
            pltpu.VMEM((5, tiles, LANES), F32),
            pltpu.VMEM((3, 4, tiles, LANES), F32),
            pltpu.VMEM((turns, 5 * tiles, LANES), F32),
            pltpu.VMEM((turns, 5 * tiles, LANES), F32),
            pltpu.VMEM((turns, lists // cores, 8, LANES), F32),
            pltpu.VMEM((turns, lists, 8, LANES), F32),
            pltpu.VMEM((turns + 8, 1, LANES), F32),
            pltpu.VMEM((turns, parts + 8, 1, LANES), F32),
        ]
        + [pltpu.SemaphoreType.DMA((turns,))] * 6,
        compiler_params=pltpu.CompilerParams(
            collective_id=0, has_side_effects=True, vmem_limit_bytes=56 * 1024 * 1024
        ),
    )(
        face_count,
        by_tile(flow_state),
        by_tile(source_term),
        volume_rate.reshape(tiles, LANES),
        face_normal.reshape(3, face_rows, LANES).transpose(1, 0, 2),
        face_owner.reshape(face_rows, LANES),
        face_neighbour.reshape(face_rows, LANES),
        send_list.reshape(lists, width // LANES, LANES),
        halo_count,
    )
    return by_component(solved), by_component(left)


def solution(mesh):
    in_specs = (
        P(None, "cells"),
        P(None, "cells"),
        P("cells"),
        P(None, ("cells", "faces")),
        P(("cells", "faces")),
        P(("cells", "faces")),
        P(("cells", "faces")),
        P("cells", None),
        P("cells"),
    )
    out_specs = (P(None, "cells"), P(None, "cells"))
    return jax.shard_map(body, mesh=mesh, in_specs=in_specs, out_specs=out_specs, check_vma=False)
```

```python
import functools

import jax
import jax.numpy as jnp
from jax import lax
from jax.experimental import pallas as pl
from jax.experimental.pallas import tpu as pltpu
from jax.sharding import PartitionSpec as P

ITERS = 2
LANES = 128
MESH = pl.DeviceIdType.MESH
F32 = jnp.float32
BF16 = jnp.bfloat16


def take_lanes(source, index):
    return jnp.take_along_axis(source, index, axis=1, mode="promise_in_bounds")


def split(value):
    high = value.astype(BF16).astype(F32)
    rest = value - high
    middle = rest.astype(BF16).astype(F32)
    return high, middle, rest - middle


def woven(*queues):
    steps = [((i + 0.5) / len(q), n, f) for n, q in enumerate(queues) for i, f in enumerate(q)]
    for _, _, step in sorted(steps, key=lambda item: item[:2]):
        step()


def kernel(
    parts,
    cores,
    count_hbm,
    flow_hbm,
    source_hbm,
    volume_hbm,
    normal_hbm,
    owner_hbm,
    neighbour_hbm,
    list_hbm,
    halo_count_hbm,
    solution_ref,
    residual_ref,
    flow_ref,
    source_ref,
    volume_ref,
    normal_ref,
    owner_ref,
    neighbour_ref,
    list_ref,
    count_ref,
    halo_count_ref,
    list_at,
    list_col,
    found_rows,
    input_sem,
    own_lane,
    right_lane,
    right_kind,
    own_row,
    local_row,
    face_u,
    face_s,
    face_n,
    signed_hot,
    plain_hot,
    flux_rows,
    setup_rows,
    cell_rows,
    size_cells,
    fields,
    halo_rows,
    halo_mix,
    blocks,
    vecs,
    pair_out,
    pair_in,
    halo_out,
    halo_in,
    dot_out,
    dot_in,
    pair_send,
    pair_recv,
    halo_send,
    halo_recv,
    dot_send,
    dot_recv,
):
    me = lax.axis_index("cells")
    core = lax.axis_index("faces")
    other = (core + 1) % cores
    tiles = volume_ref.shape[0]
    pairs = tiles // 2
    groups = pairs // 8
    cells = tiles * LANES
    lists, width = list_ref.shape
    halves = width // LANES
    side = lists // 2
    lists_here = lists // cores
    period = halo_rows.shape[0] // (4 * halves)
    turns = pair_in.shape[0]

    def fetched(number, source, target):
        copy = pltpu.make_async_copy(source, target, input_sem.at[number])
        copy.start()
        return copy

    first_copies = [
        fetched(7, halo_count_hbm, halo_count_ref),
        fetched(6, list_hbm, list_ref),
        fetched(2, flow_hbm, flow_ref),
        fetched(4, source_hbm, source_ref),
        fetched(5, volume_hbm, volume_ref),
    ]
    index_copies = [
        fetched(8, count_hbm, count_ref),
        fetched(0, owner_hbm, owner_ref),
        fetched(1, neighbour_hbm, neighbour_ref),
    ]
    normals = [fetched(3, normal_hbm, normal_ref.at[pl.ds(0, 3 * pairs)])]

    barrier = pltpu.get_barrier_semaphore()

    def signal_entry(cell, face):
        pl.semaphore_signal(
            barrier,
            inc=1,
            device_id={"cells": cell, "faces": face},
            device_id_type=MESH,
        )

    for place in range(1, parts):
        offset = (place + 1) // 2 if place % 2 else parts - place // 2
        cell = lax.rem(me + offset, parts)
        for c in range(cores):
            signal_entry(cell, c)
    for step in range(1, cores):
        signal_entry(me, lax.rem(core + step, cores))

    row8 = lax.broadcasted_iota(jnp.int32, (8, LANES), 0)

    def look_up(which, half, wanted, hs, first):
        number = len(wanted)
        at = pl.ds(8 * (halves * which + half), 8)
        row, col = list_at[at, :], list_col[at, :]
        masks = [row == row8 + 8 * h for h in hs]
        for b, field in enumerate(wanted):
            place = pl.ds(8 * (halves * number * which + number * half + b), 8)
            found = jnp.zeros((8, LANES), F32) if first else found_rows[place, :]
            for h, mask in zip(hs, masks):
                found = jnp.where(mask, take_lanes(field(h), col), found)
            found_rows[place, :] = found

    def listed(which, place, number, limit, fills):
        rows = []
        for half in range(halves):
            used = lax.broadcasted_iota(jnp.int32, (1, LANES), 1) + half * LANES < limit
            for b, fill in enumerate(fills):
                at = pl.ds(8 * (halves * number * place + number * half + b), 8)
                found = jnp.sum(found_rows[at, :], axis=0, keepdims=True)
                rows.append(jnp.where(used, found, fill))
        return rows

    def send_halo(turn, rows, place):
        pitch = 8 if turn == 0 else 16
        for k in range(lists):
            offset = k + 1 if k < side else side - 1 - k
            for c in range(cores):
                pltpu.make_async_remote_copy(
                    src_ref=halo_out.at[turn, k, pl.ds(0, rows)],
                    dst_ref=halo_in.at[turn, place, pl.ds(k * pitch, rows)],
                    send_sem=halo_send.at[turn],
                    recv_sem=halo_recv.at[turn],
                    device_id={"cells": lax.rem(me + offset + parts, parts), "faces": c},
                    device_id_type=MESH,
                ).start()

    def halo_part(turn):
        if turn == 0:
            return halo_in.at[turn, 0, pl.ds(0, 8 * lists)]
        return halo_in.at[turn] if turn == 1 else halo_in.at[turn, 0]

    def wait_halo(turn):
        part = halo_part(turn)
        pltpu.make_async_copy(part, part, halo_recv.at[turn]).wait()

    def halo_row(turn, place, row):
        pitch = 8 if turn == 0 else 16
        return halo_in[turn, place, pl.ds(row, lists, stride=pitch), :]

    def halo_sums(turn, number):
        return [
            [
                halo_row(turn, 0, half * number + b) + halo_row(turn, 1, half * number + b)
                for half in range(halves)
            ]
            for b in range(number)
        ]

    def look_up_all(turn, number, hs, first):
        def step(k, half):
            wanted = [functools.partial(partial_field, turn, b) for b in range(number)]
            return lambda: look_up(k, half, wanted, hs, first)

        return [step(k, half) for k in range(lists) for half in range(halves)]

    def put_listed(turn, fills):
        number = len(fills)
        rows = 8 if number * halves <= 8 else 16
        for k in range(lists):
            found = listed(k, k, number, halo_count_ref[k], fills)
            spare = rows - len(found)
            if spare:
                found.append(jnp.zeros((spare, LANES), F32))
            halo_out[turn, k, :rows] = jnp.concatenate(found, axis=0)
        return rows

    def pair_copy(turn, rows):
        part = pl.ds(0, rows)
        copy = pltpu.make_async_remote_copy(
            src_ref=pair_out.at[turn, part],
            dst_ref=pair_in.at[turn, part],
            send_sem=pair_send.at[turn],
            recv_sem=pair_recv.at[turn],
            device_id={"cells": me, "faces": other},
            device_id_type=MESH,
        )
        copy.start()
        return copy

    def start_dots(turn, partials):
        at = lax.broadcasted_iota(jnp.int32, (1, LANES), 1)
        packed = jnp.zeros((1, LANES), F32)
        for d, p in enumerate(partials):
            row = jnp.sum(p.reshape(tiles // 8, 8, LANES).sum(axis=0), axis=0, keepdims=True)
            packed = jnp.where(at == d, jnp.sum(row, axis=1, keepdims=True), packed)
        dot_out[turn] = packed

        @pl.when(core == 0)
        def _():
            dot_in[turn, me] = packed
            for place in range(1, parts):
                offset = (place + 1) // 2 if place % 2 else parts - place // 2
                for c in range(cores):
                    send_dots(turn, lax.rem(me + offset, parts), c)
            for c in range(1, cores):
                send_dots(turn, me, c)

    def send_dots(turn, cell, face):
        pltpu.make_async_remote_copy(
            src_ref=dot_out.at[turn],
            dst_ref=dot_in.at[turn, me],
            send_sem=dot_send.at[turn],
            recv_sem=dot_recv.at[turn],
            device_id={"cells": cell, "faces": face},
            device_id_type=MESH,
        ).start()

    def wait_dots(turn, number):
        @pl.when(core == 0)
        def _():
            part = dot_in.at[turn, pl.ds(0, parts - 1)]
            pltpu.make_async_copy(part, part, dot_recv.at[turn]).wait()

        @pl.when(core != 0)
        def _():
            part = dot_in.at[turn, pl.ds(0, parts)]
            pltpu.make_async_copy(part, part, dot_recv.at[turn]).wait()

        total = dot_in[turn, 0]
        for q in range(1, parts):
            total = total + dot_in[turn, q]
        return [jnp.broadcast_to(total[:, d : d + 1], (1, LANES)) for d in range(number)]

    def put_field(values):
        for b, value in enumerate(values):
            fields[b, pl.ds(0, tiles), :] = value
            fields[b, pl.ds(tiles, 1), :] = value[0:1]

    def put_halo(values):
        for b, value in enumerate(values):
            for half in range(halves):
                halo_mix[pl.ds(halves * b + half, lists, stride=8), :] = value[half]
        for t in range(period):
            mixed = halo_mix[pl.ds(8 * (t % lists), 8), :]
            halo_rows[pl.ds(t, 8, stride=period), :] = mixed

    def sides(g, j, b):
        here = pl.ds(g * 8, 8)
        left_at = own_lane[j, here, :]
        right_at = right_lane[j, here, :]
        kind = right_kind[j, here, :]

        def of_tile(odd):
            first = 16 * g + odd
            halo_first = (16 * g) % lists + odd
            low = fields[b, pl.ds(first, 8, stride=2), :]
            high = fields[b, pl.ds(first + 1, 8, stride=2), :]
            halo_low = halo_rows[pl.ds(2 * b * period + halo_first, 8, stride=2), :]
            halo_high = halo_rows[pl.ds((2 * b + 1) * period + halo_first, 8, stride=2), :]
            left = take_lanes(low, left_at)
            right = jnp.where(
                kind < 2,
                jnp.where(kind == 0, take_lanes(low, right_at), take_lanes(high, right_at)),
                jnp.where(
                    kind == 2, take_lanes(halo_low, right_at), take_lanes(halo_high, right_at)
                ),
            )
            return left, right

        if j == 0:
            return of_tile(0)
        if j == 2:
            return of_tile(1)
        early = lax.broadcasted_iota(jnp.int32, (8, LANES), 1) < LANES // 2
        left_a, right_a = of_tile(0)
        left_b, right_b = of_tile(1)
        return jnp.where(early, left_a, left_b), jnp.where(early, right_a, right_b)

    def put_flux(ref, g, j, b, value):
        for part, piece in enumerate(split(value)):
            row = 4 * part + b if b < 4 else 12 + part
            ref[j, pl.ds(128 * g + row, 8, stride=16), :] = piece

    def tile_rows(rows_ref, u, odd):
        at = pl.ds(u * 16, 16)
        middle = rows_ref[1, at, :]
        if odd:
            middle = pltpu.roll(middle, LANES // 2, 1)
        rows = jnp.concatenate([rows_ref[2 * odd, at, :], middle], axis=1)
        return rows[:, : 3 * LANES // 2].astype(BF16)

    def added(rows, hot):
        return lax.dot_general(
            rows, hot, (((1,), (0,)), ((), ())), preferred_element_type=F32
        )

    def scatter(u, odd):
        result = added(tile_rows(flux_rows, u, odd), signed_hot[2 * u + odd])
        result = result[:8] + result[8:]
        at = u * 16 + odd * 8
        cell_rows[0, pl.ds(at, 8), :] = result[:, :LANES]
        cell_rows[1, pl.ds(at + 8, 8), :] = result[:, LANES:]

    def scatter_size(u, odd):
        rows = tile_rows(setup_rows, u, odd)
        at = u * 16 + odd * 8
        result = added(rows, signed_hot[2 * u + odd])
        low = lax.broadcasted_iota(jnp.int32, (8, 2 * LANES), 0) < 4
        summed = result[:8] + jnp.where(low, result[8:], 0.0)
        cell_rows[0, pl.ds(at, 8), :] = summed[:, :LANES]
        cell_rows[1, pl.ds(at + 8, 8), :] = summed[:, LANES:]
        size_cells[0, pl.ds(at, 8), :] = added(rows, plain_hot[2 * u + odd])[8:]
        size_cells[1, pl.ds(at + 8, 8), :] = -result[8:, LANES:]

    def collect(turn, g, number):
        def rows(cells_ref, place, first):
            return cells_ref[place, pl.ds(first, 16, stride=8), :]

        for b in range(min(number, 4)):
            first = 128 * g + b
            low = rows(cell_rows, 0, first) + rows(cell_rows, 0, first + 4)
            high = rows(cell_rows, 1, first) + rows(cell_rows, 1, first + 4)
            pair_out[turn, pl.ds(tiles * b + 16 * g, 16), :] = low + high
        if number > 4:
            pieces = [
                rows(size_cells, 0, 128 * g + row) + rows(size_cells, 1, 128 * g + row)
                for row in (4, 5, 6)
            ]
            total = pieces[0] + pieces[1] + pieces[2]
            pair_out[turn, pl.ds(4 * tiles + 16 * g, 16), :] = total
        if g == groups - 1:
            end = pl.ds(8 * tiles, 8)
            pair_out[turn, pl.ds(number * tiles, 8), :] = cell_rows[1, end, :]
            if number > 4:
                pair_out[turn, pl.ds(number * tiles + 8, 8), :] = size_cells[1, end, :]

    def wrapped(ref, turn, b):
        number = 5 if turn == 0 else 4

        def row(at):
            return ref[turn, pl.ds(number * tiles + at, 1), :]

        if b < 4:
            return row(b) + row(b + 4)
        return row(12) + row(13) + row(14)

    def partial_field(turn, b, h):
        found = pair_out[turn, pl.ds(tiles * b + 8 * h, 8), :]
        if h == 0:
            found = found + jnp.where(row8 == 0, wrapped(pair_out, turn, b), 0.0)
        return found

    def pair_sums(turn, copy, number):
        copy.wait_recv()
        first = lax.broadcasted_iota(jnp.int32, (tiles, LANES), 0) == 0
        sums = []
        for b in range(number):
            rows = pl.ds(tiles * b, tiles)
            wrap = wrapped(pair_out, turn, b) + wrapped(pair_in, turn, b)
            total = pair_out[turn, rows, :] + pair_in[turn, rows, :]
            sums.append(total + jnp.where(first, wrap, 0.0))
        return sums

    sent = []

    def flux_steps(g):
        def step(j):
            here = pl.ds(g * 8, 8)
            u = face_u[j, here, :]
            s = face_s[j, here, :]
            n = [face_n[i, j, here, :] for i in range(3)]
            both = [sides(g, j, b) for b in range(4)]
            total = [left + right for left, right in both]
            jump = [s * (right - left) for left, right in both]
            for i in range(3):
                put_flux(flux_rows, g, j, i, u * total[i] + n[i] * total[3] - jump[i])
            last = n[0] * total[0] + n[1] * total[1] + n[2] * total[2] - jump[3]
            put_flux(flux_rows, g, j, 3, last)

        return [functools.partial(step, j) for j in range(3)]

    def over_groups(turn, faces, spread, number, search):
        for stage in range(groups + 2):
            queues = []
            if stage < groups:
                queues.append(faces(stage))
            if 1 <= stage <= groups:
                queues.append(
                    [
                        functools.partial(spread, 8 * (stage - 1) + i, odd)
                        for i in range(8)
                        for odd in range(2)
                    ]
                )
            if search and stage >= 2:
                hs = [2 * (stage - 2), 2 * (stage - 2) + 1]
                if stage == 2:
                    hs = hs[1:]
                if stage == groups + 1:
                    hs = hs + [0]
                queues.append(look_up_all(turn, number, hs, stage == 2))
            woven(*queues)
            if 1 <= stage <= groups:
                collect(turn, stage - 1, number)
        if search:
            rows = put_listed(turn + 1, [0.0] * number)
            send_halo(turn + 1, rows, core)
        copy = pair_copy(turn, number * tiles + 8 * (number - 3))
        sent.append(copy)
        return copy

    def apply_matrix(turn, values):
        copy = over_groups(turn, flux_steps, scatter, 4, True)
        sums = pair_sums(turn, copy, 4)
        volume = volume_ref[...]
        return [volume * values[b] + sums[b] for b in range(4)]

    def halo_image(turn, halos):
        wait_halo(turn)
        sums = halo_sums(turn, 4)
        return [
            [halo_volume[half] * halos[b][half] + sums[b][half] for half in range(halves)]
            for b in range(4)
        ]

    def solved(w, rvd, rschur, n):
        pressure = (w[3] - (n[0] * w[0] + n[1] * w[1] + n[2] * w[2]) * rvd) * rschur
        return [(w[i] - n[i] * pressure) * rvd for i in range(3)] + [pressure]

    def precondition(w):
        return solved(w, blocks[0], blocks[1], [blocks[2 + i] for i in range(3)])

    def precondition_halo(w):
        by_half = [
            solved([w[b][half] for b in range(4)], *halo_blocks[half]) for half in range(halves)
        ]
        return [[by_half[half][b] for half in range(halves)] for b in range(4)]

    def inverse(volume, sums):
        rvd = 1.0 / (volume + sums[0] + sums[4])
        n = sums[1:4]
        norm = n[0] * n[0] + n[1] * n[1] + n[2] * n[2]
        return rvd, 1.0 / (volume + sums[4] - norm * rvd), n

    def load(which):
        return [vecs[which, b] for b in range(4)]

    def save(which, values):
        for b in range(4):
            vecs[which, b] = values[b]

    def dot(a, b):
        return a[0] * b[0] + a[1] * b[1] + a[2] * b[2] + a[3] * b[3]

    def combine(a, scale, b):
        return [x + scale * y for x, y in zip(a, b)]

    def combine_halo(a, scale, b):
        return [[x + scale * y for x, y in zip(p, q)] for p, q in zip(a, b)]

    def load_source():
        return [source_ref[pl.ds(b, tiles, stride=4), :] for b in range(4)]

    def first_field(b, h):
        if b == 7:
            return volume_ref[pl.ds(8 * h, 8), :]
        ref, component = (flow_ref, b) if b < 3 else (source_ref, b - 3)
        return ref[pl.ds(32 * h + component, 8, stride=4), :]

    for copy in first_copies:
        copy.wait()
    for k in range(lists):
        for half in range(halves):
            cell = list_ref[k : k + 1, half * LANES : (half + 1) * LANES]
            cell = jnp.broadcast_to(cell, (8, LANES))
            at = pl.ds(8 * (halves * k + half), 8)
            list_at[at, :] = cell // LANES
            list_col[at, :] = cell - cell // LANES * LANES
    every = list(range(tiles // 8))

    @pl.when(core == 0)
    def _():
        wanted = [functools.partial(first_field, b) for b in range(3)]
        for k in range(lists):
            for half in range(halves):
                look_up(k, half, wanted, every, True)
        put_listed(0, [0.0] * 3)

    @pl.when(core == cores - 1)
    def _():
        wanted = [functools.partial(first_field, b) for b in range(3, 8)]
        for k in range(lists):
            for half in range(halves):
                look_up(k, half, wanted, every, True)
        put_listed(turns, [0.0] * 4 + [1.0])

    pl.semaphore_wait(barrier, parts * cores - 1)

    @pl.when(core == 0)
    def _():
        send_halo(0, 8, 0)

    @pl.when(core == cores - 1)
    def _():
        send_halo(turns, 16, 0)

    lane = lax.broadcasted_iota(jnp.int32, (pairs, LANES), 1)
    pair_id = lax.broadcasted_iota(jnp.int32, (pairs, LANES), 0)
    late = lane >= LANES // 2
    for copy in index_copies:
        copy.wait()
    count = count_ref[0]
    for j in range(3):
        tile = 2 * pair_id + (0 if j == 0 else 1)
        if j == 1:
            tile = 2 * pair_id + late.astype(jnp.int32)
        owner = owner_ref[pl.ds(j, pairs, stride=3), :]
        beside = neighbour_ref[pl.ds(j, pairs, stride=3), :]
        live = (3 * pair_id + j) * LANES + lane < count
        is_local = beside < cells
        column = beside - tile * LANES
        column = jnp.where(column < 0, column + cells, column)
        slot = beside - cells - (tile % lists) * width
        place = jnp.where(is_local, column, slot)
        upper = place >= LANES
        own = owner - tile * LANES
        own_lane[j] = own
        right_lane[j] = jnp.where(upper, place - LANES, place)
        right_kind[j] = jnp.where(is_local, 0, 2) + upper.astype(jnp.int32)
        own_row[j] = jnp.where(live, own, -1).astype(F32)
        local_row[j] = jnp.where(live & is_local, column, -1).astype(F32)

    cell_id = lax.broadcasted_iota(jnp.int32, (LANES, LANES), 1).astype(F32).astype(BF16)
    one, zero = jnp.ones((), BF16), jnp.zeros((), BF16)

    def by_face(rows):
        flat = rows[...].reshape(3 * pairs, LANES)
        spare = -(3 * pairs) % LANES
        flat = jnp.concatenate([flat, jnp.zeros((spare, LANES), F32)], axis=0)
        return flat.T.astype(BF16)

    own_faces, local_faces = by_face(own_row), by_face(local_row)

    def hot_of(column):
        return jnp.where(cell_id == column, one, zero)

    for u in range(pairs):
        for j in range(3):
            at = j * pairs + u
            own = jnp.broadcast_to(own_faces[:, at : at + 1], (LANES, LANES))
            local = jnp.broadcast_to(local_faces[:, at : at + 1], (LANES, LANES))
            own_hot, local_hot = hot_of(own), hot_of(local)
            low = own_hot - local_hot
            high = -hot_of(local - LANES)
            plain = own_hot + local_hot
            half = LANES // 2
            if j == 1:
                places = [(2 * u, LANES, 0, half), (2 * u + 1, LANES, half, LANES)]
            else:
                places = [(2 * u + j // 2, 0, 0, LANES)]
            for tile, row, first, last in places:
                rows = slice(row, row + last - first)
                signed_hot[tile, rows, :LANES] = low[first:last]
                signed_hot[tile, rows, LANES:] = high[first:last]
                plain_hot[tile, rows, :] = plain[first:last]

    setup_rows[...] = jnp.zeros_like(setup_rows)
    flux_rows[...] = jnp.zeros_like(flux_rows)
    cell_rows[1, :8, :] = jnp.zeros((8, LANES), F32)
    size_cells[1, :8, :] = jnp.zeros((8, LANES), F32)
    for copy in normals:
        copy.wait()

    put_field([flow_ref[pl.ds(b, tiles, stride=4), :] for b in range(3)])
    wait_halo(0)
    put_halo([[halo_row(0, 0, half * 3 + b) for half in range(halves)] for b in range(3)])

    def face_steps(g):
        def step(j):
            here = pl.ds(g * 8, 8)
            n = [normal_ref[pl.ds(24 * g + j, 8, stride=3), i, :] for i in range(3)]
            both = [sides(g, j, b) for b in range(3)]
            total = [left + right for left, right in both]
            u = 0.5 * (n[0] * total[0] + n[1] * total[1] + n[2] * total[2])
            s = jnp.abs(u) + 2.0 * jnp.sqrt(n[0] * n[0] + n[1] * n[1] + n[2] * n[2])
            u, s = 0.5 * u, 0.5 * s
            n = [0.5 * n[i] for i in range(3)]
            face_u[j, here, :] = u
            face_s[j, here, :] = s
            put_flux(setup_rows, g, j, 0, u)
            for i in range(3):
                face_n[i, j, here, :] = n[i]
                put_flux(setup_rows, g, j, 1 + i, n[i])
            put_flux(setup_rows, g, j, 4, s)

        return [functools.partial(step, j) for j in range(3)]

    copy = over_groups(0, face_steps, scatter_size, 5, True)
    rvd, rschur, coupling = inverse(volume_ref[...], pair_sums(0, copy, 5))
    blocks[0] = rvd
    blocks[1] = rschur
    for i in range(3):
        blocks[2 + i] = coupling[i]

    shadow = load_source()
    pre = precondition(shadow)
    put_field(pre)
    wait_halo(turns)

    def first_halo(b):
        return [halo_row(turns, 0, half * 5 + b) for half in range(halves)]

    halo_volume = first_halo(4)
    halo_residual = [first_halo(b) for b in range(4)]
    wait_halo(1)
    sums = halo_sums(1, 5)
    halo_blocks = [
        inverse(halo_volume[half], [sums[b][half] for b in range(5)]) for half in range(halves)
    ]
    halo_pre = precondition_halo(halo_residual)
    put_halo(halo_pre)

    V, T, W, MIDDLE, SECOND, SUM = range(6)
    image = apply_matrix(1, pre)
    shadow = load_source()
    start_dots(0, [dot(shadow, shadow), dot(shadow, image)])
    save(V, image)
    pre = precondition(image)
    put_field(pre)
    halo_v = halo_image(2, halo_pre)
    halo_pre = precondition_halo(halo_v)
    put_halo(halo_pre)

    twice = apply_matrix(2, pre)
    rho, shadow_image = wait_dots(0, 2)
    alpha = rho / shadow_image
    shadow, image = load_source(), load(V)
    middle = combine(shadow, -alpha, image)
    second = combine(image, -alpha, twice)
    start_dots(
        1, [dot(second, middle), dot(second, second), dot(shadow, middle), dot(shadow, second)]
    )
    save(T, twice)
    save(MIDDLE, middle)
    save(SECOND, second)
    pre = precondition(twice)
    put_field(pre)
    halo_t = halo_image(3, halo_pre)
    halo_pre = precondition_halo(halo_t)
    put_halo(halo_pre)

    thrice = apply_matrix(3, pre)
    second_mid, second_sq, shadow_mid, shadow_second = wait_dots(1, 4)
    omega = second_mid / second_sq
    rho_next = shadow_mid - omega * shadow_second
    beta = rho_next / rho * (alpha / omega)
    shadow, image, twice, middle, second = (
        load_source(),
        load(V),
        load(T),
        load(MIDDLE),
        load(SECOND),
    )
    residual = combine(middle, -omega, second)
    image_residual = combine(second, -omega, combine(twice, -alpha, thrice))
    direction = combine(residual, beta, combine(shadow, -omega, image))
    next_image = combine(image_residual, beta, combine(image, -omega, twice))
    start_dots(2, [dot(shadow, next_image)])
    save(V, next_image)
    save(T, residual)
    save(W, image_residual)
    save(SUM, combine([alpha * x for x in shadow], omega, middle))
    save(MIDDLE, direction)
    pre = precondition(next_image)
    put_field(pre)
    halo_w = halo_image(4, halo_pre)
    halo_second = combine_halo(halo_v, -alpha, halo_t)
    halo_next = combine_halo(
        combine_halo(halo_second, -omega, combine_halo(halo_t, -alpha, halo_w)),
        beta,
        combine_halo(halo_v, -omega, halo_t),
    )
    put_halo(precondition_halo(halo_next))

    copy = over_groups(4, flux_steps, scatter, 4, False)
    (shadow_image,) = wait_dots(2, 1)
    alpha = rho_next / shadow_image
    middle = combine(load(T), -alpha, load(V))
    save(MIDDLE, combine(load(SUM), alpha, load(MIDDLE)))
    volume = volume_ref[...]
    base = combine(load(W), -alpha, [volume * v for v in pre])
    second = combine(base, -alpha, pair_sums(4, copy, 4))
    start_dots(3, [dot(second, middle), dot(second, second)])
    known = precondition(load(MIDDLE))
    pre_mid = precondition(middle)
    second_mid, second_sq = wait_dots(3, 2)
    omega = second_mid / second_sq
    for b in range(4):
        solution_ref[pl.ds(b, tiles, stride=4), :] = known[b] + omega * pre_mid[b]
        residual_ref[pl.ds(b, tiles, stride=4), :] = middle[b] - omega * second[b]

    @pl.when(core == 0)
    def _():
        part = halo_in.at[0, 0]
        pltpu.make_async_copy(part, part, halo_send.at[0]).wait()
        for turn in range(dot_in.shape[0]):
            for part in (dot_in.at[turn, pl.ds(0, parts - 1)], dot_in.at[turn, pl.ds(0, parts)]):
                pltpu.make_async_copy(part, part, dot_send.at[turn]).wait()

    @pl.when(core == cores - 1)
    def _():
        part = halo_in.at[turns]
        pltpu.make_async_copy(part, part, halo_send.at[turns]).wait()

    for turn in range(1, turns):
        part = halo_part(turn)
        pltpu.make_async_copy(part, part, halo_send.at[turn]).wait()
    for copy in sent:
        copy.wait_send()


def body(
    flow_state,
    source_term,
    volume_rate,
    face_normal,
    face_owner,
    face_neighbour,
    face_count,
    send_list,
    halo_count,
):
    parts = lax.axis_size("cells")
    cores = lax.axis_size("faces")
    cells = flow_state.shape[1]
    tiles = cells // LANES
    pairs = tiles // 2
    groups = pairs // 8
    face_rows = face_owner.shape[0] // LANES
    lists, width = send_list.shape
    period = -(-(lists + 16) // 8) * 8
    turns = 1 + 2 * ITERS

    def by_tile(field):
        return field.reshape(4, tiles, LANES).transpose(1, 0, 2).reshape(4 * tiles, LANES)

    def by_component(field):
        return field.reshape(tiles, 4, LANES).transpose(1, 0, 2).reshape(4, cells)

    vmem = pl.BlockSpec(memory_space=pltpu.VMEM)
    hbm = pl.BlockSpec(memory_space=pltpu.HBM)
    ints = pltpu.VMEM((3, pairs, LANES), jnp.int32)
    floats = pltpu.VMEM((3, pairs, LANES), F32)
    hot = pltpu.VMEM((tiles, 3 * LANES // 2, 2 * LANES), BF16)
    out = jax.ShapeDtypeStruct((4 * tiles, LANES), F32)
    solved, left = pl.pallas_call(
        functools.partial(kernel, parts, cores),
        out_shape=(out, out),
        in_specs=[hbm] * 9,
        out_specs=(vmem, vmem),
        scratch_shapes=[
            pltpu.VMEM((4 * tiles, LANES), F32),
            pltpu.VMEM((4 * tiles, LANES), F32),
            pltpu.VMEM((tiles, LANES), F32),
            pltpu.VMEM((face_rows + 8, 3, LANES), F32),
            pltpu.VMEM((face_rows, LANES), jnp.int32),
            pltpu.VMEM((face_rows, LANES), jnp.int32),
            pltpu.VMEM((lists, width), jnp.int32),
            pltpu.SMEM((1,), jnp.int32),
            pltpu.SMEM((lists,), jnp.int32),
            pltpu.VMEM((8 * lists * width // LANES, LANES), jnp.int32),
            pltpu.VMEM((8 * lists * width // LANES, LANES), jnp.int32),
            pltpu.VMEM((40 * lists * width // LANES, LANES), F32),
            pltpu.SemaphoreType.DMA((9,)),
            ints,
            ints,
            ints,
            floats,
            floats,
            floats,
            floats,
            pltpu.VMEM((3, 3, pairs, LANES), F32),
            hot,
            pltpu.VMEM((tiles, 3 * LANES // 2, LANES), BF16),
            pltpu.VMEM((3, 16 * pairs, LANES), F32),
            pltpu.VMEM((3, 16 * pairs, LANES), F32),
            pltpu.VMEM((2, 8 * tiles + 8, LANES), F32),
            pltpu.VMEM((2, 8 * tiles + 8, LANES), F32),
            pltpu.VMEM((4, tiles + 8, LANES), F32),
            pltpu.VMEM((8 * period, LANES), F32),
            pltpu.VMEM((8 * lists, LANES), F32),
            pltpu.VMEM((5, tiles, LANES), F32),
            pltpu.VMEM((6, 4, tiles, LANES), F32),
            pltpu.VMEM((turns, 5 * tiles + 16, LANES), F32),
            pltpu.VMEM((turns, 5 * tiles + 16, LANES), F32),
            pltpu.VMEM((turns + 1, lists, 16, LANES), F32),
            pltpu.VMEM((turns + 1, cores, 16 * lists, LANES), F32),
            pltpu.VMEM((turns + 8, 1, LANES), F32),
            pltpu.VMEM((turns - 1, parts + 8, 1, LANES), F32),
            pltpu.SemaphoreType.DMA((turns,)),
            pltpu.SemaphoreType.DMA((turns,)),
            pltpu.SemaphoreType.DMA((turns + 1,)),
            pltpu.SemaphoreType.DMA((turns + 1,)),
            pltpu.SemaphoreType.DMA((turns - 1,)),
            pltpu.SemaphoreType.DMA((turns - 1,)),
        ],
        compiler_params=pltpu.CompilerParams(
            collective_id=0, has_side_effects=True, vmem_limit_bytes=56 * 1024 * 1024
        ),
    )(
        face_count,
        by_tile(flow_state),
        by_tile(source_term),
        volume_rate.reshape(tiles, LANES),
        face_normal.reshape(3, face_rows, LANES).transpose(1, 0, 2),
        face_owner.reshape(face_rows, LANES),
        face_neighbour.reshape(face_rows, LANES),
        send_list,
        halo_count,
    )
    return by_component(solved), by_component(left)


def solution(mesh):
    in_specs = (
        P(None, "cells"),
        P(None, "cells"),
        P("cells"),
        P(None, ("cells", "faces")),
        P(("cells", "faces")),
        P(("cells", "faces")),
        P(("cells", "faces")),
        P("cells", None),
        P("cells"),
    )
    out_specs = (P(None, "cells"), P(None, "cells"))
    return jax.shard_map(body, mesh=mesh, in_specs=in_specs, out_specs=out_specs, check_vma=False)
```

```python
import functools

import jax
import jax.numpy as jnp
from jax import lax
from jax.experimental import pallas as pl
from jax.experimental.pallas import tpu as pltpu
from jax.sharding import PartitionSpec as P

ITERS = 2
LANES = 128
MESH = pl.DeviceIdType.MESH
F32 = jnp.float32
BF16 = jnp.bfloat16


def take_lanes(source, index):
    return jnp.take_along_axis(source, index, axis=1, mode="promise_in_bounds")


def split(value):
    high = value.astype(BF16).astype(F32)
    rest = value - high
    middle = rest.astype(BF16).astype(F32)
    return high, middle, rest - middle


def woven(*queues):
    steps = [((i + 0.5) / len(q), n, f) for n, q in enumerate(queues) for i, f in enumerate(q)]
    for _, _, step in sorted(steps, key=lambda item: item[:2]):
        step()


def kernel(
    parts,
    cores,
    count_hbm,
    flow_hbm,
    source_hbm,
    volume_hbm,
    normal_hbm,
    owner_hbm,
    neighbour_hbm,
    list_hbm,
    halo_count_hbm,
    solution_ref,
    residual_ref,
    flow_ref,
    source_ref,
    volume_ref,
    normal_ref,
    owner_ref,
    neighbour_ref,
    list_ref,
    count_ref,
    halo_count_ref,
    list_at,
    list_col,
    found_rows,
    input_sem,
    own_lane,
    right_lane,
    right_kind,
    own_row,
    local_row,
    face_u,
    face_s,
    face_n,
    signed_hot,
    own_hot,
    flux_rows,
    setup_rows,
    cell_rows,
    size_cells,
    own_cells,
    local_sums,
    fields,
    halo_rows,
    halo_mix,
    blocks,
    vecs,
    pair_out,
    pair_in,
    halo_out,
    halo_in,
    dot_out,
    dot_in,
    pair_send,
    pair_recv,
    halo_send,
    halo_recv,
    dot_send,
    dot_recv,
):
    me = lax.axis_index("cells")
    core = lax.axis_index("faces")
    other = (core + 1) % cores
    tiles = volume_ref.shape[0]
    pairs = tiles // 2
    groups = pairs // 8
    cells = tiles * LANES
    lists, width = list_ref.shape
    halves = width // LANES
    side = lists // 2
    lists_here = lists // cores
    period = halo_rows.shape[0] // (4 * halves)
    turns = pair_in.shape[0]
    offsets = [k + 1 if k < side else side - 1 - k for k in range(lists)]
    sooner = [k for k in range(lists) if offsets[k] % 2]
    later = [k for k in range(lists) if offsets[k] % 2 == 0]

    def fetched(number, source, target):
        copy = pltpu.make_async_copy(source, target, input_sem.at[number])
        copy.start()
        return copy

    first_copies = [
        fetched(7, halo_count_hbm, halo_count_ref),
        fetched(6, list_hbm, list_ref),
        fetched(2, flow_hbm, flow_ref),
        fetched(4, source_hbm, source_ref),
        fetched(5, volume_hbm, volume_ref),
    ]
    index_copies = [
        fetched(8, count_hbm, count_ref),
        fetched(0, owner_hbm, owner_ref),
        fetched(1, neighbour_hbm, neighbour_ref),
    ]
    normals = [fetched(3, normal_hbm, normal_ref.at[pl.ds(0, 3 * pairs)])]

    barrier = pltpu.get_barrier_semaphore()

    def signal_entry(cell, face):
        pl.semaphore_signal(
            barrier,
            inc=1,
            device_id={"cells": cell, "faces": face},
            device_id_type=MESH,
        )

    for place in range(1, parts):
        offset = (place + 1) // 2 if place % 2 else parts - place // 2
        cell = lax.rem(me + offset, parts)
        for c in range(cores):
            signal_entry(cell, c)
    for step in range(1, cores):
        signal_entry(me, lax.rem(core + step, cores))

    row8 = lax.broadcasted_iota(jnp.int32, (8, LANES), 0)

    def look_up(which, half, wanted, hs, first):
        number = len(wanted)
        at = pl.ds(8 * (halves * which + half), 8)
        row, col = list_at[at, :], list_col[at, :]
        masks = [row == row8 + 8 * h for h in hs]
        for b, field in enumerate(wanted):
            place = pl.ds(8 * (halves * number * which + number * half + b), 8)
            found = jnp.zeros((8, LANES), F32) if first else found_rows[place, :]
            for h, mask in zip(hs, masks):
                found = jnp.where(mask, take_lanes(field(h), col), found)
            found_rows[place, :] = found

    def row_sums(blocks_of):
        shift, level = 1, blocks_of
        while len(level) > 1:
            mask = (row8 // shift) % 2 == 0
            level = [
                jnp.where(mask, x, y) + pltpu.roll(jnp.where(mask, y, x), 8 - shift, 0)
                for x, y in zip(level[::2], level[1::2])
            ]
            shift *= 2
        return level[0]

    def listed(k, fills):
        number = len(fills)
        flat = [found_rows[pl.ds(8 * (halves * number * k + i), 8), :] for i in range(halves * number)]
        flat += [jnp.zeros((8, LANES), F32)] * (-len(flat) % 8)
        slot = lax.broadcasted_iota(jnp.int32, (8, LANES), 1)
        limit = halo_count_ref[k]
        tiles_of = []
        for first in range(0, len(flat), 8):
            row = row8 + first
            half = row // number
            used = slot + half * LANES < limit
            fill = jnp.zeros((8, LANES), F32)
            if fills[-1]:
                fill = jnp.where(row % number == number - 1, fills[-1], 0.0)
            tiles_of.append(jnp.where(used, row_sums(flat[first : first + 8]), fill))
        return tiles_of

    def send_halo(turn, rows, place, which):
        pitch = 8 if turn == 0 else 16
        for k in which:
            for c in range(cores):
                pltpu.make_async_remote_copy(
                    src_ref=halo_out.at[turn, k, pl.ds(0, rows)],
                    dst_ref=halo_in.at[turn, place, pl.ds(k * pitch, rows)],
                    send_sem=halo_send.at[turn],
                    recv_sem=halo_recv.at[turn],
                    device_id={"cells": lax.rem(me + offsets[k] + parts, parts), "faces": c},
                    device_id_type=MESH,
                ).start()

    def halo_part(turn):
        if turn == 0:
            return halo_in.at[turn, 0, pl.ds(0, 8 * lists)]
        return halo_in.at[turn] if turn == 1 else halo_in.at[turn, 0]

    def wait_halo(turn):
        part = halo_part(turn)
        pltpu.make_async_copy(part, part, halo_recv.at[turn]).wait()

    def halo_row(turn, place, row):
        pitch = 8 if turn == 0 else 16
        return halo_in[turn, place, pl.ds(row, lists, stride=pitch), :]

    def halo_sums(turn, number):
        return [
            [
                halo_row(turn, 0, half * number + b) + halo_row(turn, 1, half * number + b)
                for half in range(halves)
            ]
            for b in range(number)
        ]

    def look_up_all(turn, number, hs, first, which):
        def step(k, half):
            wanted = [functools.partial(partial_field, turn, b) for b in range(number)]
            return lambda: look_up(k, half, wanted, hs, first)

        return [step(k, half) for k in which for half in range(halves)]

    def put_listed(turn, fills, which):
        for k in which:
            for i, rows in enumerate(listed(k, fills)):
                halo_out[turn, k, pl.ds(8 * i, 8)] = rows
        return 8 * (-(-halves * len(fills) // 8))

    def pair_copy(turn, rows):
        part = pl.ds(0, rows)
        copy = pltpu.make_async_remote_copy(
            src_ref=pair_out.at[turn, part],
            dst_ref=pair_in.at[turn, part],
            send_sem=pair_send.at[turn],
            recv_sem=pair_recv.at[turn],
            device_id={"cells": me, "faces": other},
            device_id_type=MESH,
        )
        copy.start()
        return copy

    def start_dots(turn, partials):
        at = lax.broadcasted_iota(jnp.int32, (1, LANES), 1)
        packed = jnp.zeros((1, LANES), F32)
        for d, p in enumerate(partials):
            row = jnp.sum(p.reshape(tiles // 8, 8, LANES).sum(axis=0), axis=0, keepdims=True)
            packed = jnp.where(at == d, jnp.sum(row, axis=1, keepdims=True), packed)
        dot_out[turn] = packed

        @pl.when(core == 0)
        def _():
            dot_in[turn, me] = packed
            for place in range(1, parts):
                offset = (place + 1) // 2 if place % 2 else parts - place // 2
                for c in range(cores):
                    send_dots(turn, lax.rem(me + offset, parts), c)
            for c in range(1, cores):
                send_dots(turn, me, c)

    def send_dots(turn, cell, face):
        pltpu.make_async_remote_copy(
            src_ref=dot_out.at[turn],
            dst_ref=dot_in.at[turn, me],
            send_sem=dot_send.at[turn],
            recv_sem=dot_recv.at[turn],
            device_id={"cells": cell, "faces": face},
            device_id_type=MESH,
        ).start()

    def wait_dots(turn, number):
        @pl.when(core == 0)
        def _():
            part = dot_in.at[turn, pl.ds(0, parts - 1)]
            pltpu.make_async_copy(part, part, dot_recv.at[turn]).wait()

        @pl.when(core != 0)
        def _():
            part = dot_in.at[turn, pl.ds(0, parts)]
            pltpu.make_async_copy(part, part, dot_recv.at[turn]).wait()

        total = dot_in[turn, 0]
        for q in range(1, parts):
            total = total + dot_in[turn, q]
        return [jnp.broadcast_to(total[:, d : d + 1], (1, LANES)) for d in range(number)]

    def put_field(values):
        for b, value in enumerate(values):
            fields[b, pl.ds(0, tiles), :] = value
            fields[b, pl.ds(tiles, 1), :] = value[0:1]

    def put_halo(values):
        for b, value in enumerate(values):
            for half in range(halves):
                halo_mix[pl.ds(halves * b + half, lists, stride=8), :] = value[half]
        for t in range(period):
            mixed = halo_mix[pl.ds(8 * (t % lists), 8), :]
            halo_rows[pl.ds(t, 8, stride=period), :] = mixed

    def by_tile(g, j, of_tile):
        if j == 0:
            return of_tile(0)
        if j == 2:
            return of_tile(1)
        early = lax.broadcasted_iota(jnp.int32, (8, LANES), 1) < LANES // 2
        return [jnp.where(early, x, y) for x, y in zip(of_tile(0), of_tile(1))]

    def local_sides(g, j, b):
        here = pl.ds(g * 8, 8)
        left_at = own_lane[j, here, :]
        right_at = right_lane[j, here, :]
        kind = right_kind[j, here, :]

        def of_tile(odd):
            first = 16 * g + odd
            low = fields[b, pl.ds(first, 8, stride=2), :]
            high = fields[b, pl.ds(first + 1, 8, stride=2), :]
            right = jnp.where(
                kind == 0,
                take_lanes(low, right_at),
                jnp.where(kind == 1, take_lanes(high, right_at), 0.0),
            )
            return [take_lanes(low, left_at), right]

        return by_tile(g, j, of_tile)

    def halo_side(g, j, b):
        here = pl.ds(g * 8, 8)
        right_at = right_lane[j, here, :]
        kind = right_kind[j, here, :]

        def of_tile(odd):
            first = (16 * g) % lists + odd
            low = halo_rows[pl.ds(2 * b * period + first, 8, stride=2), :]
            high = halo_rows[pl.ds((2 * b + 1) * period + first, 8, stride=2), :]
            right = jnp.where(
                kind == 2,
                take_lanes(low, right_at),
                jnp.where(kind == 3, take_lanes(high, right_at), 0.0),
            )
            return [right]

        return by_tile(g, j, of_tile)[0]

    def put_flux(ref, g, j, b, value):
        for part, piece in enumerate(split(value)):
            row = 4 * part + b if b < 4 else 12 + part
            ref[j, pl.ds(128 * g + row, 8, stride=16), :] = piece

    def tile_rows(rows_ref, u, odd):
        at = pl.ds(u * 16, 16)
        middle = rows_ref[1, at, :]
        if odd:
            middle = pltpu.roll(middle, LANES // 2, 1)
        rows = jnp.concatenate([rows_ref[2 * odd, at, :], middle], axis=1)
        return rows[:, : 3 * LANES // 2].astype(BF16)

    def added(rows, hot):
        return lax.dot_general(
            rows, hot, (((1,), (0,)), ((), ())), preferred_element_type=F32
        )

    def put_cells(u, odd, low, high):
        at = u * 16 + odd * 8
        cell_rows[0, pl.ds(at, 8), :] = low
        cell_rows[1, pl.ds(at + 8, 8), :] = high

    def scatter(u):
        for odd in range(2):
            result = added(tile_rows(flux_rows, u, odd), signed_hot[2 * u + odd])
            result = result[:8] + result[8:]
            put_cells(u, odd, result[:, :LANES], result[:, LANES:])

    def own_sums(rows, u):
        result = added(jnp.concatenate(rows, axis=0), own_hot[u])
        return [result[16 * odd : 16 * odd + 16, odd * LANES : (odd + 1) * LANES] for odd in range(2)]

    def scatter_halo(u):
        rows = [tile_rows(flux_rows, u, odd) for odd in range(2)]
        for odd, result in enumerate(own_sums(rows, u)):
            own_cells[pl.ds(u * 16 + odd * 8, 8), :] = result[:8] + result[8:]

    def scatter_size(u):
        rows = [tile_rows(setup_rows, u, odd) for odd in range(2)]
        own = own_sums(rows, u)
        for odd in range(2):
            at = u * 16 + odd * 8
            result = added(rows[odd], signed_hot[2 * u + odd])
            low = lax.broadcasted_iota(jnp.int32, (8, 2 * LANES), 0) < 4
            summed = result[:8] + jnp.where(low, result[8:], 0.0)
            put_cells(u, odd, summed[:, :LANES], summed[:, LANES:])
            size_cells[0, pl.ds(at, 8), :] = 2.0 * own[odd][8:] - result[8:, :LANES]
            size_cells[1, pl.ds(at + 8, 8), :] = -result[8:, LANES:]

    def cell_sums(g, b):
        def rows(place, first):
            return cell_rows[place, pl.ds(first, 16, stride=8), :]

        first = 128 * g + b
        return rows(0, first) + rows(0, first + 4) + (rows(1, first) + rows(1, first + 4))

    def collect_local(g):
        for b in range(4):
            local_sums[pl.ds(tiles * b + 16 * g, 16), :] = cell_sums(g, b)

    def collect_halo(turn, g):
        for b in range(4):
            first = 128 * g + b
            here = pl.ds(tiles * b + 16 * g, 16)
            halo = own_cells[pl.ds(first, 16, stride=8), :]
            halo = halo + own_cells[pl.ds(first + 4, 16, stride=8), :]
            pair_out[turn, here, :] = local_sums[here, :] + halo
        if g == groups - 1:
            pair_out[turn, pl.ds(4 * tiles, 8), :] = cell_rows[1, pl.ds(8 * tiles, 8), :]

    def collect_setup(g):
        for b in range(4):
            local_sums[pl.ds(tiles * b + 16 * g, 16), :] = cell_sums(g, b)
        pieces = [
            size_cells[place, pl.ds(128 * g + row, 16, stride=8), :]
            for place in range(2)
            for row in (4, 5, 6)
        ]
        local_sums[pl.ds(4 * tiles + 16 * g, 16), :] = functools.reduce(jnp.add, pieces)

    def collect_setup_halo(g):
        for b in range(5):
            here = pl.ds(tiles * b + 16 * g, 16)
            total = local_sums[here, :]
            if b in (0, 4):
                first = 128 * g + b // 4
                total = total + own_cells[pl.ds(first, 16, stride=8), :]
                total = total + own_cells[pl.ds(first + 4, 16, stride=8), :]
            pair_out[0, here, :] = total
        if g == groups - 1:
            end = pl.ds(8 * tiles, 8)
            pair_out[0, pl.ds(5 * tiles, 8), :] = cell_rows[1, end, :]
            pair_out[0, pl.ds(5 * tiles + 8, 8), :] = size_cells[1, end, :]

    def wrapped(ref, turn, b):
        number = 5 if turn == 0 else 4

        def row(at):
            return ref[turn, pl.ds(number * tiles + at, 1), :]

        if b < 4:
            return row(b) + row(b + 4)
        return row(12) + row(13) + row(14)

    def partial_field(turn, b, h):
        found = pair_out[turn, pl.ds(tiles * b + 8 * h, 8), :]
        if h == 0:
            found = found + jnp.where(row8 == 0, wrapped(pair_out, turn, b), 0.0)
        return found

    def pair_sums(turn, copy, number):
        copy.wait_recv()
        first = lax.broadcasted_iota(jnp.int32, (tiles, LANES), 0) == 0
        sums = []
        for b in range(number):
            rows = pl.ds(tiles * b, tiles)
            wrap = wrapped(pair_out, turn, b) + wrapped(pair_in, turn, b)
            total = pair_out[turn, rows, :] + pair_in[turn, rows, :]
            sums.append(total + jnp.where(first, wrap, 0.0))
        return sums

    sent = []

    def coefficients(g, j):
        here = pl.ds(g * 8, 8)
        n = [face_n[i, j, here, :] for i in range(3)]
        return face_u[j, here, :], face_s[j, here, :], n

    def put_fluxes(g, j, u, n, total, jump):
        for i in range(3):
            put_flux(flux_rows, g, j, i, u * total[i] + n[i] * total[3] - jump[i])
        last = n[0] * total[0] + n[1] * total[1] + n[2] * total[2] - jump[3]
        put_flux(flux_rows, g, j, 3, last)

    def local_steps(g):
        def step(j):
            u, s, n = coefficients(g, j)
            both = [local_sides(g, j, b) for b in range(4)]
            total = [left + right for left, right in both]
            jump = [s * (right - left) for left, right in both]
            put_fluxes(g, j, u, n, total, jump)

        return [functools.partial(step, j) for j in range(3)]

    def halo_steps(g):
        def step(j):
            u, s, n = coefficients(g, j)
            right = [halo_side(g, j, b) for b in range(4)]
            put_fluxes(g, j, u, n, right, [s * r for r in right])

        return [functools.partial(step, j) for j in range(3)]

    def over_groups(faces, spread, collect, turn=None, number=4):
        for stage in range(groups + 1 if turn is None else groups + 2):
            queues = []
            if stage < groups:
                queues.append(faces(stage))
            if 1 <= stage <= groups:
                first = 8 * (stage - 1)
                queues.append([functools.partial(spread, first + i) for i in range(8)])
            if turn is not None and stage >= 2:
                hs = [2 * (stage - 2), 2 * (stage - 2) + 1]
                if stage == 2:
                    hs = hs[1:]
                if stage == groups + 1:
                    hs = hs + [0]
                queues.append(look_up_all(turn, number, hs, stage == 2, sooner))
            woven(*queues)
            if 1 <= stage <= groups:
                collect(stage - 1)

    def sent_sums(turn, number, last=False):
        fills = [0.0] * number
        if not last:
            rows = put_listed(turn + 1, fills, sooner)
            send_halo(turn + 1, rows, core, sooner)
        copy = pair_copy(turn, number * tiles + 8 * (number - 3))
        sent.append(copy)
        if not last:
            for step in look_up_all(turn, number, list(range(tiles // 8)), True, later):
                step()
            put_listed(turn + 1, fills, later)
            send_halo(turn + 1, rows, core, later)
        return copy

    def start_matrix(values):
        put_field(values)
        over_groups(local_steps, scatter, collect_local)

    def finish_matrix(turn, halos, last=False):
        put_halo(halos)
        collect = functools.partial(collect_halo, turn)
        over_groups(halo_steps, scatter_halo, collect, None if last else turn)
        return sent_sums(turn, 4, last)

    def image_of(turn, copy, values):
        sums = pair_sums(turn, copy, 4)
        volume = volume_ref[...]
        return [volume * values[b] + sums[b] for b in range(4)]

    def halo_image(turn, halos):
        wait_halo(turn)
        sums = halo_sums(turn, 4)
        return [
            [halo_volume[half] * halos[b][half] + sums[b][half] for half in range(halves)]
            for b in range(4)
        ]

    def solved(w, rvd, rschur, n):
        pressure = (w[3] - (n[0] * w[0] + n[1] * w[1] + n[2] * w[2]) * rvd) * rschur
        return [(w[i] - n[i] * pressure) * rvd for i in range(3)] + [pressure]

    def precondition(w):
        return solved(w, blocks[0], blocks[1], [blocks[2 + i] for i in range(3)])

    def precondition_halo(w):
        by_half = [
            solved([w[b][half] for b in range(4)], *halo_blocks[half]) for half in range(halves)
        ]
        return [[by_half[half][b] for half in range(halves)] for b in range(4)]

    def inverse(volume, sums):
        rvd = 1.0 / (volume + sums[0] + sums[4])
        n = sums[1:4]
        norm = n[0] * n[0] + n[1] * n[1] + n[2] * n[2]
        return rvd, 1.0 / (volume + sums[4] - norm * rvd), n

    def load(which):
        return [vecs[which, b] for b in range(4)]

    def save(which, values):
        for b in range(4):
            vecs[which, b] = values[b]

    def dot(a, b):
        return a[0] * b[0] + a[1] * b[1] + a[2] * b[2] + a[3] * b[3]

    def combine(a, scale, b):
        return [x + scale * y for x, y in zip(a, b)]

    def combine_halo(a, scale, b):
        return [[x + scale * y for x, y in zip(p, q)] for p, q in zip(a, b)]

    def load_source():
        return [source_ref[pl.ds(b, tiles, stride=4), :] for b in range(4)]

    def first_field(b, h):
        if b == 7:
            return volume_ref[pl.ds(8 * h, 8), :]
        ref, component = (flow_ref, b) if b < 3 else (source_ref, b - 3)
        return ref[pl.ds(32 * h + component, 8, stride=4), :]

    for copy in first_copies:
        copy.wait()
    for k in range(lists):
        for half in range(halves):
            cell = list_ref[k : k + 1, half * LANES : (half + 1) * LANES]
            cell = jnp.broadcast_to(cell, (8, LANES))
            at = pl.ds(8 * (halves * k + half), 8)
            list_at[at, :] = cell // LANES
            list_col[at, :] = cell - cell // LANES * LANES
    every = list(range(tiles // 8))
    every_list = list(range(lists))

    @pl.when(core == 0)
    def _():
        wanted = [functools.partial(first_field, b) for b in range(3)]
        for k in range(lists):
            for half in range(halves):
                look_up(k, half, wanted, every, True)
        put_listed(0, [0.0] * 3, every_list)

    @pl.when(core == cores - 1)
    def _():
        wanted = [functools.partial(first_field, b) for b in range(3, 8)]
        for k in range(lists):
            for half in range(halves):
                look_up(k, half, wanted, every, True)
        put_listed(turns, [0.0] * 4 + [1.0], every_list)

    pl.semaphore_wait(barrier, parts * cores - 1)

    @pl.when(core == 0)
    def _():
        send_halo(0, 8, 0, sooner + later)

    @pl.when(core == cores - 1)
    def _():
        send_halo(turns, 16, 0, sooner + later)

    lane = lax.broadcasted_iota(jnp.int32, (pairs, LANES), 1)
    pair_id = lax.broadcasted_iota(jnp.int32, (pairs, LANES), 0)
    late = lane >= LANES // 2
    for copy in index_copies:
        copy.wait()
    count = count_ref[0]
    for j in range(3):
        tile = 2 * pair_id + (0 if j == 0 else 1)
        if j == 1:
            tile = 2 * pair_id + late.astype(jnp.int32)
        owner = owner_ref[pl.ds(j, pairs, stride=3), :]
        beside = neighbour_ref[pl.ds(j, pairs, stride=3), :]
        live = (3 * pair_id + j) * LANES + lane < count
        is_local = beside < cells
        column = beside - tile * LANES
        column = jnp.where(column < 0, column + cells, column)
        slot = beside - cells - (tile % lists) * width
        place = jnp.where(is_local, column, slot)
        upper = place >= LANES
        own = owner - tile * LANES
        own_lane[j] = own
        right_lane[j] = jnp.where(upper, place - LANES, place)
        right_kind[j] = jnp.where(is_local, 0, 2) + upper.astype(jnp.int32)
        own_row[j] = jnp.where(live, own, -1).astype(F32)
        local_row[j] = jnp.where(live & is_local, column, -1).astype(F32)

    cell_id = lax.broadcasted_iota(jnp.int32, (LANES, LANES), 1).astype(F32).astype(BF16)
    one, zero = jnp.ones((), BF16), jnp.zeros((), BF16)

    def by_face(rows):
        flat = rows[...].reshape(3 * pairs, LANES)
        spare = -(3 * pairs) % LANES
        flat = jnp.concatenate([flat, jnp.zeros((spare, LANES), F32)], axis=0)
        return flat.T.astype(BF16)

    own_faces, local_faces = by_face(own_row), by_face(local_row)

    def hot_of(column):
        return jnp.where(cell_id == column, one, zero)

    for u in range(pairs):
        for j in range(3):
            at = j * pairs + u
            own = jnp.broadcast_to(own_faces[:, at : at + 1], (LANES, LANES))
            local = jnp.broadcast_to(local_faces[:, at : at + 1], (LANES, LANES))
            own_cell = hot_of(own)
            low = own_cell - hot_of(local)
            high = -hot_of(local - LANES)
            half = LANES // 2
            if j == 1:
                places = [(2 * u, LANES, 0, half), (2 * u + 1, LANES, half, LANES)]
            else:
                places = [(2 * u + j // 2, 0, 0, LANES)]
            for tile, row, first, last in places:
                rows = slice(row, row + last - first)
                signed_hot[tile, rows, :LANES] = low[first:last]
                signed_hot[tile, rows, LANES:] = high[first:last]
                lanes = slice(tile % 2 * LANES, (tile % 2 + 1) * LANES)
                own_hot[u, rows, lanes] = own_cell[first:last]

    setup_rows[...] = jnp.zeros_like(setup_rows)
    flux_rows[...] = jnp.zeros_like(flux_rows)
    cell_rows[1, :8, :] = jnp.zeros((8, LANES), F32)
    size_cells[1, :8, :] = jnp.zeros((8, LANES), F32)
    for copy in normals:
        copy.wait()

    put_field([flow_ref[pl.ds(b, tiles, stride=4), :] for b in range(3)])
    def face_steps(g):
        def step(j):
            here = pl.ds(g * 8, 8)
            inside = right_kind[j, here, :] < 2
            n = [normal_ref[pl.ds(24 * g + j, 8, stride=3), i, :] for i in range(3)]
            both = [local_sides(g, j, b) for b in range(3)]
            total = [left + right for left, right in both]
            u = 0.25 * (n[0] * total[0] + n[1] * total[1] + n[2] * total[2])
            size = jnp.sqrt(n[0] * n[0] + n[1] * n[1] + n[2] * n[2])
            face_u[j, here, :] = u
            face_s[j, here, :] = size
            put_flux(setup_rows, g, j, 0, jnp.where(inside, u, 0.0))
            for i in range(3):
                half = 0.5 * n[i]
                face_n[i, j, here, :] = half
                put_flux(setup_rows, g, j, 1 + i, half)
            put_flux(setup_rows, g, j, 4, jnp.where(inside, jnp.abs(u) + size, 0.0))

        return [functools.partial(step, j) for j in range(3)]

    def face_halo_steps(g):
        def step(j):
            here = pl.ds(g * 8, 8)
            outside = right_kind[j, here, :] >= 2
            u, size, n = coefficients(g, j)
            right = [halo_side(g, j, b) for b in range(3)]
            u = u + 0.5 * (n[0] * right[0] + n[1] * right[1] + n[2] * right[2])
            s = jnp.abs(u) + size
            face_u[j, here, :] = u
            face_s[j, here, :] = s
            put_flux(flux_rows, g, j, 0, jnp.where(outside, u, 0.0))
            put_flux(flux_rows, g, j, 1, jnp.where(outside, s, 0.0))

        return [functools.partial(step, j) for j in range(3)]

    over_groups(face_steps, scatter_size, collect_setup)
    wait_halo(0)
    put_halo([[halo_row(0, 0, half * 3 + b) for half in range(halves)] for b in range(3)])

    over_groups(face_halo_steps, scatter_halo, collect_setup_halo, 0, 5)
    copy = sent_sums(0, 5)
    rvd, rschur, coupling = inverse(volume_ref[...], pair_sums(0, copy, 5))
    blocks[0] = rvd
    blocks[1] = rschur
    for i in range(3):
        blocks[2 + i] = coupling[i]

    shadow = load_source()
    pre = precondition(shadow)
    start_matrix(pre)
    wait_halo(turns)

    def first_halo(b):
        return [halo_row(turns, 0, half * 5 + b) for half in range(halves)]

    halo_volume = first_halo(4)
    halo_residual = [first_halo(b) for b in range(4)]
    wait_halo(1)
    sums = halo_sums(1, 5)
    halo_blocks = [
        inverse(halo_volume[half], [sums[b][half] for b in range(5)]) for half in range(halves)
    ]
    halo_pre = precondition_halo(halo_residual)

    V, T, W, MIDDLE, SECOND, SUM = range(6)
    copy = finish_matrix(1, halo_pre)
    image = image_of(1, copy, pre)
    shadow = load_source()
    start_dots(0, [dot(shadow, shadow), dot(shadow, image)])
    save(V, image)
    pre = precondition(image)
    start_matrix(pre)
    halo_v = halo_image(2, halo_pre)
    halo_pre = precondition_halo(halo_v)

    copy = finish_matrix(2, halo_pre)
    twice = image_of(2, copy, pre)
    rho, shadow_image = wait_dots(0, 2)
    alpha = rho / shadow_image
    shadow, image = load_source(), load(V)
    middle = combine(shadow, -alpha, image)
    second = combine(image, -alpha, twice)
    start_dots(
        1, [dot(second, middle), dot(second, second), dot(shadow, middle), dot(shadow, second)]
    )
    save(T, twice)
    save(MIDDLE, middle)
    save(SECOND, second)
    pre = precondition(twice)
    start_matrix(pre)
    halo_t = halo_image(3, halo_pre)
    halo_pre = precondition_halo(halo_t)

    copy = finish_matrix(3, halo_pre)
    thrice = image_of(3, copy, pre)
    second_mid, second_sq, shadow_mid, shadow_second = wait_dots(1, 4)
    omega = second_mid / second_sq
    rho_next = shadow_mid - omega * shadow_second
    beta = rho_next / rho * (alpha / omega)
    shadow, image, twice, middle, second = (
        load_source(),
        load(V),
        load(T),
        load(MIDDLE),
        load(SECOND),
    )
    residual = combine(middle, -omega, second)
    image_residual = combine(second, -omega, combine(twice, -alpha, thrice))
    direction = combine(residual, beta, combine(shadow, -omega, image))
    next_image = combine(image_residual, beta, combine(image, -omega, twice))
    start_dots(2, [dot(shadow, next_image)])
    save(V, next_image)
    save(T, residual)
    save(W, image_residual)
    save(SUM, combine([alpha * x for x in shadow], omega, middle))
    save(MIDDLE, direction)
    pre = precondition(next_image)
    start_matrix(pre)
    halo_w = halo_image(4, halo_pre)
    halo_second = combine_halo(halo_v, -alpha, halo_t)
    halo_next = combine_halo(
        combine_halo(halo_second, -omega, combine_halo(halo_t, -alpha, halo_w)),
        beta,
        combine_halo(halo_v, -omega, halo_t),
    )
    copy = finish_matrix(4, precondition_halo(halo_next), last=True)
    (shadow_image,) = wait_dots(2, 1)
    alpha = rho_next / shadow_image
    middle = combine(load(T), -alpha, load(V))
    save(MIDDLE, combine(load(SUM), alpha, load(MIDDLE)))
    volume = volume_ref[...]
    base = combine(load(W), -alpha, [volume * v for v in pre])
    second = combine(base, -alpha, pair_sums(4, copy, 4))
    start_dots(3, [dot(second, middle), dot(second, second)])
    known = precondition(load(MIDDLE))
    pre_mid = precondition(middle)
    second_mid, second_sq = wait_dots(3, 2)
    omega = second_mid / second_sq
    for b in range(4):
        solution_ref[pl.ds(b, tiles, stride=4), :] = known[b] + omega * pre_mid[b]
        residual_ref[pl.ds(b, tiles, stride=4), :] = middle[b] - omega * second[b]

    @pl.when(core == 0)
    def _():
        part = halo_in.at[0, 0]
        pltpu.make_async_copy(part, part, halo_send.at[0]).wait()
        for turn in range(dot_in.shape[0]):
            for part in (dot_in.at[turn, pl.ds(0, parts - 1)], dot_in.at[turn, pl.ds(0, parts)]):
                pltpu.make_async_copy(part, part, dot_send.at[turn]).wait()

    @pl.when(core == cores - 1)
    def _():
        part = halo_in.at[turns]
        pltpu.make_async_copy(part, part, halo_send.at[turns]).wait()

    for turn in range(1, turns):
        part = halo_part(turn)
        pltpu.make_async_copy(part, part, halo_send.at[turn]).wait()
    for copy in sent:
        copy.wait_send()


def body(
    flow_state,
    source_term,
    volume_rate,
    face_normal,
    face_owner,
    face_neighbour,
    face_count,
    send_list,
    halo_count,
):
    parts = lax.axis_size("cells")
    cores = lax.axis_size("faces")
    cells = flow_state.shape[1]
    tiles = cells // LANES
    pairs = tiles // 2
    groups = pairs // 8
    face_rows = face_owner.shape[0] // LANES
    lists, width = send_list.shape
    period = -(-(lists + 16) // 8) * 8
    turns = 1 + 2 * ITERS

    def by_tile(field):
        return field.reshape(4, tiles, LANES).transpose(1, 0, 2).reshape(4 * tiles, LANES)

    def by_component(field):
        return field.reshape(tiles, 4, LANES).transpose(1, 0, 2).reshape(4, cells)

    vmem = pl.BlockSpec(memory_space=pltpu.VMEM)
    hbm = pl.BlockSpec(memory_space=pltpu.HBM)
    ints = pltpu.VMEM((3, pairs, LANES), jnp.int32)
    floats = pltpu.VMEM((3, pairs, LANES), F32)
    hot = pltpu.VMEM((tiles, 3 * LANES // 2, 2 * LANES), BF16)
    out = pltpu.VMEM((4 * tiles, LANES), F32)
    solved, left = pl.pallas_call(
        functools.partial(kernel, parts, cores),
        out_shape=(out, out),
        in_specs=[hbm] * 9,
        out_specs=(vmem, vmem),
        scratch_shapes=[
            pltpu.VMEM((4 * tiles, LANES), F32),
            pltpu.VMEM((4 * tiles, LANES), F32),
            pltpu.VMEM((tiles, LANES), F32),
            pltpu.VMEM((face_rows + 8, 3, LANES), F32),
            pltpu.VMEM((face_rows, LANES), jnp.int32),
            pltpu.VMEM((face_rows, LANES), jnp.int32),
            pltpu.VMEM((lists, width), jnp.int32),
            pltpu.SMEM((1,), jnp.int32),
            pltpu.SMEM((lists,), jnp.int32),
            pltpu.VMEM((8 * lists * width // LANES, LANES), jnp.int32),
            pltpu.VMEM((8 * lists * width // LANES, LANES), jnp.int32),
            pltpu.VMEM((40 * lists * width // LANES, LANES), F32),
            pltpu.SemaphoreType.DMA((9,)),
            ints,
            ints,
            ints,
            floats,
            floats,
            floats,
            floats,
            pltpu.VMEM((3, 3, pairs, LANES), F32),
            hot,
            pltpu.VMEM((pairs, 3 * LANES // 2, 2 * LANES), BF16),
            pltpu.VMEM((3, 16 * pairs, LANES), F32),
            pltpu.VMEM((3, 16 * pairs, LANES), F32),
            pltpu.VMEM((2, 8 * tiles + 8, LANES), F32),
            pltpu.VMEM((2, 8 * tiles + 8, LANES), F32),
            pltpu.VMEM((8 * tiles, LANES), F32),
            pltpu.VMEM((5 * tiles, LANES), F32),
            pltpu.VMEM((4, tiles + 8, LANES), F32),
            pltpu.VMEM((8 * period, LANES), F32),
            pltpu.VMEM((8 * lists, LANES), F32),
            pltpu.VMEM((5, tiles, LANES), F32),
            pltpu.VMEM((6, 4, tiles, LANES), F32),
            pltpu.VMEM((turns, 5 * tiles + 16, LANES), F32),
            pltpu.VMEM((turns, 5 * tiles + 16, LANES), F32),
            pltpu.VMEM((turns + 1, lists, 16, LANES), F32),
            pltpu.VMEM((turns + 1, cores, 16 * lists, LANES), F32),
            pltpu.VMEM((turns + 8, 1, LANES), F32),
            pltpu.VMEM((turns - 1, parts + 8, 1, LANES), F32),
            pltpu.SemaphoreType.DMA((turns,)),
            pltpu.SemaphoreType.DMA((turns,)),
            pltpu.SemaphoreType.DMA((turns + 1,)),
            pltpu.SemaphoreType.DMA((turns + 1,)),
            pltpu.SemaphoreType.DMA((turns - 1,)),
            pltpu.SemaphoreType.DMA((turns - 1,)),
        ],
        compiler_params=pltpu.CompilerParams(
            collective_id=0, has_side_effects=True, vmem_limit_bytes=56 * 1024 * 1024
        ),
    )(
        face_count,
        by_tile(flow_state),
        by_tile(source_term),
        volume_rate.reshape(tiles, LANES),
        face_normal.reshape(3, face_rows, LANES).transpose(1, 0, 2),
        face_owner.reshape(face_rows, LANES),
        face_neighbour.reshape(face_rows, LANES),
        send_list,
        halo_count,
    )
    return by_component(solved), by_component(left)


def solution(mesh):
    in_specs = (
        P(None, "cells"),
        P(None, "cells"),
        P("cells"),
        P(None, ("cells", "faces")),
        P(("cells", "faces")),
        P(("cells", "faces")),
        P(("cells", "faces")),
        P("cells", None),
        P("cells"),
    )
    out_specs = (P(None, "cells"), P(None, "cells"))
    return jax.shard_map(body, mesh=mesh, in_specs=in_specs, out_specs=out_specs, check_vma=False)
```

```python
import functools

import jax
import jax.numpy as jnp
from jax import lax
from jax.experimental import pallas as pl
from jax.experimental.pallas import tpu as pltpu
from jax.sharding import PartitionSpec as P

ITERS = 2
LANES = 128
MESH = pl.DeviceIdType.MESH
F32 = jnp.float32
BF16 = jnp.bfloat16


def take_lanes(source, index):
    return jnp.take_along_axis(source, index, axis=1, mode="promise_in_bounds")


def split(value):
    high = value.astype(BF16).astype(F32)
    rest = value - high
    middle = rest.astype(BF16).astype(F32)
    return high, middle, rest - middle


def woven(*queues):
    steps = [((i + 0.5) / len(q), n, f) for n, q in enumerate(queues) for i, f in enumerate(q)]
    for _, _, step in sorted(steps, key=lambda item: item[:2]):
        step()


def kernel(
    parts,
    cores,
    count_hbm,
    flow_hbm,
    source_hbm,
    volume_hbm,
    normal_hbm,
    owner_hbm,
    neighbour_hbm,
    list_hbm,
    halo_count_hbm,
    out_ref,
    flow_ref,
    source_ref,
    volume_ref,
    normal_ref,
    owner_ref,
    neighbour_ref,
    list_ref,
    count_ref,
    halo_count_ref,
    list_at,
    list_col,
    found_rows,
    input_sem,
    own_lane,
    right_lane,
    right_kind,
    own_row,
    local_row,
    face_u,
    face_s,
    face_n,
    signed_hot,
    own_hot,
    flux_rows,
    setup_rows,
    cell_rows,
    size_cells,
    own_cells,
    local_sums,
    fields,
    halo_rows,
    blocks,
    vecs,
    pair_out,
    pair_in,
    halo_out,
    halo_in,
    dot_out,
    dot_in,
    pair_send,
    pair_recv,
    halo_send,
    halo_recv,
    dot_send,
    dot_recv,
):
    me = lax.axis_index("cells")
    core = lax.axis_index("faces")
    other = (core + 1) % cores
    tiles = volume_ref.shape[0]
    pairs = tiles // 2
    groups = pairs // 8
    cells = tiles * LANES
    lists, width = list_ref.shape
    halves = width // LANES
    side = lists // 2
    lists_here = lists // cores
    period = halo_rows.shape[0] // (4 * halves)
    turns = pair_in.shape[0]
    offsets = [k + 1 if k < side else side - 1 - k for k in range(lists)]
    sooner = [k for k in range(lists) if offsets[k] % 2]
    later = [k for k in range(lists) if offsets[k] % 2 == 0]

    def fetched(number, source, target):
        copy = pltpu.make_async_copy(source, target, input_sem.at[number])
        copy.start()
        return copy

    first_copies = [
        fetched(7, halo_count_hbm, halo_count_ref),
        fetched(6, list_hbm, list_ref),
        fetched(2, flow_hbm, flow_ref),
        fetched(4, source_hbm, source_ref),
        fetched(5, volume_hbm, volume_ref),
    ]
    index_copies = [
        fetched(8, count_hbm, count_ref),
        fetched(0, owner_hbm, owner_ref),
        fetched(1, neighbour_hbm, neighbour_ref),
    ]
    normals = [fetched(3, normal_hbm, normal_ref.at[pl.ds(0, 3 * pairs)])]

    barrier = pltpu.get_barrier_semaphore()

    def signal_entry(cell, face):
        pl.semaphore_signal(
            barrier,
            inc=1,
            device_id={"cells": cell, "faces": face},
            device_id_type=MESH,
        )

    for place in range(1, parts):
        offset = (place + 1) // 2 if place % 2 else parts - place // 2
        cell = lax.rem(me + offset, parts)
        for c in range(cores):
            signal_entry(cell, c)
    for step in range(1, cores):
        signal_entry(me, lax.rem(core + step, cores))

    row8 = lax.broadcasted_iota(jnp.int32, (8, LANES), 0)

    def look_up(which, half, wanted, hs, first):
        number = len(wanted)
        at = pl.ds(8 * (halves * which + half), 8)
        row, col = list_at[at, :], list_col[at, :]
        masks = [row == row8 + 8 * h for h in hs]
        for b, field in enumerate(wanted):
            place = pl.ds(8 * (halves * number * which + number * half + b), 8)
            found = jnp.zeros((8, LANES), F32) if first else found_rows[place, :]
            for h, mask in zip(hs, masks):
                found = jnp.where(mask, take_lanes(field(h), col), found)
            found_rows[place, :] = found

    def row_sums(blocks_of):
        shift, level = 1, blocks_of
        while len(level) > 1:
            mask = (row8 // shift) % 2 == 0
            level = [
                jnp.where(mask, x, y) + pltpu.roll(jnp.where(mask, y, x), 8 - shift, 0)
                for x, y in zip(level[::2], level[1::2])
            ]
            shift *= 2
        return level[0]

    def listed(k, fills):
        number = len(fills)
        flat = [found_rows[pl.ds(8 * (halves * number * k + i), 8), :] for i in range(halves * number)]
        flat += [jnp.zeros((8, LANES), F32)] * (-len(flat) % 8)
        slot = lax.broadcasted_iota(jnp.int32, (8, LANES), 1)
        limit = halo_count_ref[k]
        tiles_of = []
        for first in range(0, len(flat), 8):
            row = row8 + first
            half = row // number
            used = slot + half * LANES < limit
            fill = jnp.zeros((8, LANES), F32)
            if fills[-1]:
                fill = jnp.where(row % number == number - 1, fills[-1], 0.0)
            tiles_of.append(jnp.where(used, row_sums(flat[first : first + 8]), fill))
        return tiles_of

    def send_halo(turn, rows, place, which):
        pitch = 8 if turn == 0 else 16
        for k in which:
            for c in range(cores):
                pltpu.make_async_remote_copy(
                    src_ref=halo_out.at[turn, k, pl.ds(0, rows)],
                    dst_ref=halo_in.at[turn, place, pl.ds(k * pitch, rows)],
                    send_sem=halo_send.at[turn],
                    recv_sem=halo_recv.at[turn],
                    device_id={"cells": lax.rem(me + offsets[k] + parts, parts), "faces": c},
                    device_id_type=MESH,
                ).start()

    def halo_part(turn):
        if turn == 0:
            return halo_in.at[turn, 0, pl.ds(0, 8 * lists)]
        return halo_in.at[turn] if turn == 1 else halo_in.at[turn, 0]

    def wait_halo(turn):
        part = halo_part(turn)
        pltpu.make_async_copy(part, part, halo_recv.at[turn]).wait()

    def halo_row(turn, place, row):
        pitch = 8 if turn == 0 else 16
        return halo_in[turn, place, pl.ds(row, lists, stride=pitch), :]

    def halo_sums(turn, number):
        return [
            [
                halo_row(turn, 0, half * number + b) + halo_row(turn, 1, half * number + b)
                for half in range(halves)
            ]
            for b in range(number)
        ]

    def look_up_all(turn, number, hs, first, which):
        def step(k, half):
            wanted = [functools.partial(partial_field, turn, b) for b in range(number)]
            return lambda: look_up(k, half, wanted, hs, first)

        return [step(k, half) for k in which for half in range(halves)]

    def put_listed(turn, fills, which):
        for k in which:
            for i, rows in enumerate(listed(k, fills)):
                halo_out[turn, k, pl.ds(8 * i, 8)] = rows
        return 8 * (-(-halves * len(fills) // 8))

    def pair_copy(turn, rows):
        part = pl.ds(0, rows)
        copy = pltpu.make_async_remote_copy(
            src_ref=pair_out.at[turn, part],
            dst_ref=pair_in.at[turn, part],
            send_sem=pair_send.at[turn],
            recv_sem=pair_recv.at[turn],
            device_id={"cells": me, "faces": other},
            device_id_type=MESH,
        )
        copy.start()
        return copy

    def start_dots(turn, partials):
        at = lax.broadcasted_iota(jnp.int32, (1, LANES), 1)
        packed = jnp.zeros((1, LANES), F32)
        for d, p in enumerate(partials):
            row = jnp.sum(p.reshape(tiles // 8, 8, LANES).sum(axis=0), axis=0, keepdims=True)
            packed = jnp.where(at == d, jnp.sum(row, axis=1, keepdims=True), packed)
        dot_out[turn] = packed

        @pl.when(core == 0)
        def _():
            dot_in[turn, me] = packed
            for place in range(1, parts):
                offset = (place + 1) // 2 if place % 2 else parts - place // 2
                for c in range(cores):
                    send_dots(turn, lax.rem(me + offset, parts), c)
            for c in range(1, cores):
                send_dots(turn, me, c)

    def send_dots(turn, cell, face):
        pltpu.make_async_remote_copy(
            src_ref=dot_out.at[turn],
            dst_ref=dot_in.at[turn, me],
            send_sem=dot_send.at[turn],
            recv_sem=dot_recv.at[turn],
            device_id={"cells": cell, "faces": face},
            device_id_type=MESH,
        ).start()

    def wait_dots(turn, number):
        @pl.when(core == 0)
        def _():
            part = dot_in.at[turn, pl.ds(0, parts - 1)]
            pltpu.make_async_copy(part, part, dot_recv.at[turn]).wait()

        @pl.when(core != 0)
        def _():
            part = dot_in.at[turn, pl.ds(0, parts)]
            pltpu.make_async_copy(part, part, dot_recv.at[turn]).wait()

        total = dot_in[turn, 0]
        for q in range(1, parts):
            total = total + dot_in[turn, q]
        return [jnp.broadcast_to(total[:, d : d + 1], (1, LANES)) for d in range(number)]

    def put_field(values):
        for b, value in enumerate(values):
            fields[b, pl.ds(0, tiles), :] = value
            fields[b, pl.ds(tiles, 1), :] = value[0:1]

    def put_halo(values):
        for b, value in enumerate(values):
            for half in range(halves):
                rows = jnp.concatenate([value[half]] * (-(-period // lists)), axis=0)
                halo_rows[pl.ds((halves * b + half) * period, period), :] = rows[:period]

    def by_tile(g, j, of_tile):
        if j == 0:
            return of_tile(0)
        if j == 2:
            return of_tile(1)
        early = lax.broadcasted_iota(jnp.int32, (8, LANES), 1) < LANES // 2
        return [jnp.where(early, x, y) for x, y in zip(of_tile(0), of_tile(1))]

    def local_sides(g, j, b):
        here = pl.ds(g * 8, 8)
        left_at = own_lane[j, here, :]
        right_at = right_lane[j, here, :]
        kind = right_kind[j, here, :]

        def of_tile(odd):
            first = 16 * g + odd
            low = fields[b, pl.ds(first, 8, stride=2), :]
            high = fields[b, pl.ds(first + 1, 8, stride=2), :]
            right = jnp.where(
                kind == 0,
                take_lanes(low, right_at),
                jnp.where(kind == 1, take_lanes(high, right_at), 0.0),
            )
            return [take_lanes(low, left_at), right]

        return by_tile(g, j, of_tile)

    def halo_side(g, j, b):
        here = pl.ds(g * 8, 8)
        right_at = right_lane[j, here, :]
        kind = right_kind[j, here, :]

        def of_tile(odd):
            first = (16 * g) % lists + odd
            low = halo_rows[pl.ds(2 * b * period + first, 8, stride=2), :]
            high = halo_rows[pl.ds((2 * b + 1) * period + first, 8, stride=2), :]
            right = jnp.where(
                kind == 2,
                take_lanes(low, right_at),
                jnp.where(kind == 3, take_lanes(high, right_at), 0.0),
            )
            return [right]

        return by_tile(g, j, of_tile)[0]

    def put_flux(ref, g, j, b, value):
        for part, piece in enumerate(split(value)):
            row = 4 * part + b if b < 4 else 12 + part
            ref[row // 8, j, pl.ds(64 * g + row % 8, 8, stride=8), :] = piece

    def tile_rows(rows_ref, u, odd):
        at = pl.ds(u * 8, 8)
        pieces = []
        for half in range(2):
            middle = rows_ref[half, 1, at, :]
            if odd:
                middle = pltpu.roll(middle, LANES // 2, 1)
            pieces.append(jnp.concatenate([rows_ref[half, 2 * odd, at, :], middle], axis=1))
        return jnp.concatenate(pieces, axis=0)[:, : 3 * LANES // 2].astype(BF16)

    def added(rows, hot):
        return lax.dot_general(
            rows, hot, (((1,), (0,)), ((), ())), preferred_element_type=F32
        )

    def put_cells(u, odd, low, high):
        at = u * 16 + odd * 8
        cell_rows[0, pl.ds(at, 8), :] = low
        cell_rows[1, pl.ds(at + 8, 8), :] = high

    def scatter(u):
        for odd in range(2):
            result = added(tile_rows(flux_rows, u, odd), signed_hot[2 * u + odd])
            result = result[:8] + result[8:]
            put_cells(u, odd, result[:, :LANES], result[:, LANES:])

    def own_sums(rows, u):
        result = added(jnp.concatenate(rows, axis=0), own_hot[u])
        return [result[16 * odd : 16 * odd + 16, odd * LANES : (odd + 1) * LANES] for odd in range(2)]

    def scatter_halo(u):
        rows = [tile_rows(flux_rows, u, odd) for odd in range(2)]
        for odd, result in enumerate(own_sums(rows, u)):
            own_cells[pl.ds(u * 16 + odd * 8, 8), :] = result[:8] + result[8:]

    def scatter_size(u):
        rows = [tile_rows(setup_rows, u, odd) for odd in range(2)]
        own = own_sums(rows, u)
        for odd in range(2):
            at = u * 16 + odd * 8
            result = added(rows[odd], signed_hot[2 * u + odd])
            low = lax.broadcasted_iota(jnp.int32, (8, 2 * LANES), 0) < 4
            summed = result[:8] + jnp.where(low, result[8:], 0.0)
            put_cells(u, odd, summed[:, :LANES], summed[:, LANES:])
            size_cells[0, pl.ds(at, 8), :] = 2.0 * own[odd][8:] - result[8:, :LANES]
            size_cells[1, pl.ds(at + 8, 8), :] = -result[8:, LANES:]

    def cell_sums(g, b):
        def rows(place, first):
            return cell_rows[place, pl.ds(first, 16, stride=8), :]

        first = 128 * g + b
        return rows(0, first) + rows(0, first + 4) + (rows(1, first) + rows(1, first + 4))

    def collect_local(g):
        for b in range(4):
            local_sums[pl.ds(tiles * b + 16 * g, 16), :] = cell_sums(g, b)

    def collect_halo(turn, g):
        for b in range(4):
            first = 128 * g + b
            here = pl.ds(tiles * b + 16 * g, 16)
            halo = own_cells[pl.ds(first, 16, stride=8), :]
            halo = halo + own_cells[pl.ds(first + 4, 16, stride=8), :]
            pair_out[turn, here, :] = local_sums[here, :] + halo
        if g == groups - 1:
            pair_out[turn, pl.ds(4 * tiles, 8), :] = cell_rows[1, pl.ds(8 * tiles, 8), :]

    def collect_setup(g):
        for b in range(4):
            local_sums[pl.ds(tiles * b + 16 * g, 16), :] = cell_sums(g, b)
        pieces = [
            size_cells[place, pl.ds(128 * g + row, 16, stride=8), :]
            for place in range(2)
            for row in (4, 5, 6)
        ]
        local_sums[pl.ds(4 * tiles + 16 * g, 16), :] = functools.reduce(jnp.add, pieces)

    def collect_setup_halo(g):
        for b in range(5):
            here = pl.ds(tiles * b + 16 * g, 16)
            total = local_sums[here, :]
            if b in (0, 4):
                first = 128 * g + b // 4
                total = total + own_cells[pl.ds(first, 16, stride=8), :]
                total = total + own_cells[pl.ds(first + 4, 16, stride=8), :]
            pair_out[0, here, :] = total
        if g == groups - 1:
            end = pl.ds(8 * tiles, 8)
            pair_out[0, pl.ds(5 * tiles, 8), :] = cell_rows[1, end, :]
            pair_out[0, pl.ds(5 * tiles + 8, 8), :] = size_cells[1, end, :]

    def wrapped(ref, turn, b):
        number = 5 if turn == 0 else 4

        def row(at):
            return ref[turn, pl.ds(number * tiles + at, 1), :]

        if b < 4:
            return row(b) + row(b + 4)
        return row(12) + row(13) + row(14)

    def partial_field(turn, b, h):
        found = pair_out[turn, pl.ds(tiles * b + 8 * h, 8), :]
        if h == 0:
            found = found + jnp.where(row8 == 0, wrapped(pair_out, turn, b), 0.0)
        return found

    def pair_sums(turn, copy, number):
        copy.wait_recv()
        first = lax.broadcasted_iota(jnp.int32, (tiles, LANES), 0) == 0
        sums = []
        for b in range(number):
            rows = pl.ds(tiles * b, tiles)
            wrap = wrapped(pair_out, turn, b) + wrapped(pair_in, turn, b)
            total = pair_out[turn, rows, :] + pair_in[turn, rows, :]
            sums.append(total + jnp.where(first, wrap, 0.0))
        return sums

    sent = []

    def coefficients(g, j):
        here = pl.ds(g * 8, 8)
        n = [face_n[i, j, here, :] for i in range(3)]
        return face_u[j, here, :], face_s[j, here, :], n

    def put_fluxes(g, j, u, n, total, jump):
        for i in range(3):
            put_flux(flux_rows, g, j, i, u * total[i] + n[i] * total[3] - jump[i])
        last = n[0] * total[0] + n[1] * total[1] + n[2] * total[2] - jump[3]
        put_flux(flux_rows, g, j, 3, last)

    def local_steps(g):
        def step(j):
            u, s, n = coefficients(g, j)
            both = [local_sides(g, j, b) for b in range(4)]
            total = [left + right for left, right in both]
            jump = [s * (right - left) for left, right in both]
            put_fluxes(g, j, u, n, total, jump)

        return [functools.partial(step, j) for j in range(3)]

    def halo_steps(g):
        def step(j):
            u, s, n = coefficients(g, j)
            right = [halo_side(g, j, b) for b in range(4)]
            put_fluxes(g, j, u, n, right, [s * r for r in right])

        return [functools.partial(step, j) for j in range(3)]

    def over_groups(faces, spread, collect, turn=None, number=4):
        for stage in range(groups + 1 if turn is None else groups + 2):
            queues = []
            if stage < groups:
                queues.append(faces(stage))
            if 1 <= stage <= groups:
                first = 8 * (stage - 1)
                queues.append([functools.partial(spread, first + i) for i in range(8)])
            if turn is not None and stage >= 2:
                hs = [2 * (stage - 2), 2 * (stage - 2) + 1]
                if stage == 2:
                    hs = hs[1:]
                if stage == groups + 1:
                    hs = hs + [0]
                queues.append(look_up_all(turn, number, hs, stage == 2, sooner))
            woven(*queues)
            if 1 <= stage <= groups:
                collect(stage - 1)

    def sent_sums(turn, number, last=False):
        fills = [0.0] * number
        if not last:
            rows = put_listed(turn + 1, fills, sooner)
            send_halo(turn + 1, rows, core, sooner)
        copy = pair_copy(turn, number * tiles + 8 * (number - 3))
        sent.append(copy)
        if not last:
            for step in look_up_all(turn, number, list(range(tiles // 8)), True, later):
                step()
            put_listed(turn + 1, fills, later)
            send_halo(turn + 1, rows, core, later)
        return copy

    def start_matrix(values):
        put_field(values)
        over_groups(local_steps, scatter, collect_local)

    def finish_matrix(turn, halos, last=False):
        put_halo(halos)
        collect = functools.partial(collect_halo, turn)
        over_groups(halo_steps, scatter_halo, collect, None if last else turn)
        return sent_sums(turn, 4, last)

    def image_of(turn, copy, values):
        sums = pair_sums(turn, copy, 4)
        volume = volume_ref[...]
        return [volume * values[b] + sums[b] for b in range(4)]

    def halo_image(turn, halos):
        wait_halo(turn)
        sums = halo_sums(turn, 4)
        return [
            [halo_volume[half] * halos[b][half] + sums[b][half] for half in range(halves)]
            for b in range(4)
        ]

    def solved(w, rvd, rschur, n):
        pressure = (w[3] - (n[0] * w[0] + n[1] * w[1] + n[2] * w[2]) * rvd) * rschur
        return [(w[i] - n[i] * pressure) * rvd for i in range(3)] + [pressure]

    def precondition(w):
        return solved(w, blocks[0], blocks[1], [blocks[2 + i] for i in range(3)])

    def precondition_halo(w):
        by_half = [
            solved([w[b][half] for b in range(4)], *halo_blocks[half]) for half in range(halves)
        ]
        return [[by_half[half][b] for half in range(halves)] for b in range(4)]

    def inverse(volume, sums):
        rvd = 1.0 / (volume + sums[0] + sums[4])
        n = sums[1:4]
        norm = n[0] * n[0] + n[1] * n[1] + n[2] * n[2]
        return rvd, 1.0 / (volume + sums[4] - norm * rvd), n

    def load(which):
        return [vecs[which, b] for b in range(4)]

    def save(which, values):
        for b in range(4):
            vecs[which, b] = values[b]

    def dot(a, b):
        return a[0] * b[0] + a[1] * b[1] + a[2] * b[2] + a[3] * b[3]

    def combine(a, scale, b):
        return [x + scale * y for x, y in zip(a, b)]

    def combine_halo(a, scale, b):
        return [[x + scale * y for x, y in zip(p, q)] for p, q in zip(a, b)]

    def load_source():
        return [source_ref[pl.ds(b, tiles, stride=4), :] for b in range(4)]

    def first_field(b, h):
        if b == 7:
            return volume_ref[pl.ds(8 * h, 8), :]
        ref, component = (flow_ref, b) if b < 3 else (source_ref, b - 3)
        return ref[pl.ds(32 * h + component, 8, stride=4), :]

    for copy in first_copies:
        copy.wait()
    for k in range(lists):
        for half in range(halves):
            cell = list_ref[k : k + 1, half * LANES : (half + 1) * LANES]
            cell = jnp.broadcast_to(cell, (8, LANES))
            at = pl.ds(8 * (halves * k + half), 8)
            list_at[at, :] = cell // LANES
            list_col[at, :] = cell - cell // LANES * LANES
    every = list(range(tiles // 8))
    every_list = list(range(lists))

    @pl.when(core == 0)
    def _():
        wanted = [functools.partial(first_field, b) for b in range(3)]
        for k in range(lists):
            for half in range(halves):
                look_up(k, half, wanted, every, True)
        put_listed(0, [0.0] * 3, every_list)

    @pl.when(core == cores - 1)
    def _():
        wanted = [functools.partial(first_field, b) for b in range(3, 8)]
        for k in range(lists):
            for half in range(halves):
                look_up(k, half, wanted, every, True)
        put_listed(turns, [0.0] * 4 + [1.0], every_list)

    pl.semaphore_wait(barrier, parts * cores - 1)

    @pl.when(core == 0)
    def _():
        send_halo(0, 8, 0, sooner + later)

    @pl.when(core == cores - 1)
    def _():
        send_halo(turns, 16, 0, sooner + later)

    lane = lax.broadcasted_iota(jnp.int32, (pairs, LANES), 1)
    pair_id = lax.broadcasted_iota(jnp.int32, (pairs, LANES), 0)
    late = lane >= LANES // 2
    for copy in index_copies:
        copy.wait()
    count = count_ref[0]
    for j in range(3):
        tile = 2 * pair_id + (0 if j == 0 else 1)
        if j == 1:
            tile = 2 * pair_id + late.astype(jnp.int32)
        owner = owner_ref[pl.ds(j, pairs, stride=3), :]
        beside = neighbour_ref[pl.ds(j, pairs, stride=3), :]
        live = (3 * pair_id + j) * LANES + lane < count
        is_local = beside < cells
        column = beside - tile * LANES
        column = jnp.where(column < 0, column + cells, column)
        slot = beside - cells - (tile % lists) * width
        place = jnp.where(is_local, column, slot)
        upper = place >= LANES
        own = owner - tile * LANES
        own_lane[j] = own
        right_lane[j] = jnp.where(upper, place - LANES, place)
        right_kind[j] = jnp.where(is_local, 0, 2) + upper.astype(jnp.int32)
        own_row[j] = jnp.where(live, own, -1).astype(F32)
        local_row[j] = jnp.where(live & is_local, column, -1).astype(F32)

    cell_id = lax.broadcasted_iota(jnp.int32, (LANES, LANES), 1).astype(F32).astype(BF16)
    one, zero = jnp.ones((), BF16), jnp.zeros((), BF16)

    def by_face(rows):
        flat = rows[...].reshape(3 * pairs, LANES)
        spare = -(3 * pairs) % LANES
        flat = jnp.concatenate([flat, jnp.zeros((spare, LANES), F32)], axis=0)
        return flat.T.astype(BF16)

    own_faces, local_faces = by_face(own_row), by_face(local_row)

    def hot_of(column):
        return jnp.where(cell_id == column, one, zero)

    for u in range(pairs):
        for j in range(3):
            at = j * pairs + u
            own = jnp.broadcast_to(own_faces[:, at : at + 1], (LANES, LANES))
            local = jnp.broadcast_to(local_faces[:, at : at + 1], (LANES, LANES))
            own_cell = hot_of(own)
            low = own_cell - hot_of(local)
            high = -hot_of(local - LANES)
            half = LANES // 2
            if j == 1:
                places = [(2 * u, LANES, 0, half), (2 * u + 1, LANES, half, LANES)]
            else:
                places = [(2 * u + j // 2, 0, 0, LANES)]
            for tile, row, first, last in places:
                rows = slice(row, row + last - first)
                signed_hot[tile, rows, :LANES] = low[first:last]
                signed_hot[tile, rows, LANES:] = high[first:last]
                lanes = slice(tile % 2 * LANES, (tile % 2 + 1) * LANES)
                own_hot[u, rows, lanes] = own_cell[first:last]

    setup_rows[...] = jnp.zeros_like(setup_rows)
    flux_rows[...] = jnp.zeros_like(flux_rows)
    cell_rows[1, :8, :] = jnp.zeros((8, LANES), F32)
    size_cells[1, :8, :] = jnp.zeros((8, LANES), F32)
    for copy in normals:
        copy.wait()

    put_field([flow_ref[pl.ds(b, tiles, stride=4), :] for b in range(3)])
    def face_steps(g):
        def step(j):
            here = pl.ds(g * 8, 8)
            inside = right_kind[j, here, :] < 2
            n = [normal_ref[pl.ds(24 * g + j, 8, stride=3), i, :] for i in range(3)]
            both = [local_sides(g, j, b) for b in range(3)]
            total = [left + right for left, right in both]
            u = 0.25 * (n[0] * total[0] + n[1] * total[1] + n[2] * total[2])
            size = jnp.sqrt(n[0] * n[0] + n[1] * n[1] + n[2] * n[2])
            face_u[j, here, :] = u
            face_s[j, here, :] = size
            put_flux(setup_rows, g, j, 0, jnp.where(inside, u, 0.0))
            for i in range(3):
                half = 0.5 * n[i]
                face_n[i, j, here, :] = half
                put_flux(setup_rows, g, j, 1 + i, half)
            put_flux(setup_rows, g, j, 4, jnp.where(inside, jnp.abs(u) + size, 0.0))

        return [functools.partial(step, j) for j in range(3)]

    def face_halo_steps(g):
        def step(j):
            here = pl.ds(g * 8, 8)
            outside = right_kind[j, here, :] >= 2
            u, size, n = coefficients(g, j)
            right = [halo_side(g, j, b) for b in range(3)]
            u = u + 0.5 * (n[0] * right[0] + n[1] * right[1] + n[2] * right[2])
            s = jnp.abs(u) + size
            face_u[j, here, :] = u
            face_s[j, here, :] = s
            put_flux(flux_rows, g, j, 0, jnp.where(outside, u, 0.0))
            put_flux(flux_rows, g, j, 1, jnp.where(outside, s, 0.0))

        return [functools.partial(step, j) for j in range(3)]

    over_groups(face_steps, scatter_size, collect_setup)
    wait_halo(0)
    put_halo([[halo_row(0, 0, half * 3 + b) for half in range(halves)] for b in range(3)])

    over_groups(face_halo_steps, scatter_halo, collect_setup_halo, 0, 5)
    copy = sent_sums(0, 5)
    rvd, rschur, coupling = inverse(volume_ref[...], pair_sums(0, copy, 5))
    blocks[0] = rvd
    blocks[1] = rschur
    for i in range(3):
        blocks[2 + i] = coupling[i]

    shadow = load_source()
    pre = precondition(shadow)
    start_matrix(pre)
    wait_halo(turns)

    def first_halo(b):
        return [halo_row(turns, 0, half * 5 + b) for half in range(halves)]

    halo_volume = first_halo(4)
    halo_residual = [first_halo(b) for b in range(4)]
    wait_halo(1)
    sums = halo_sums(1, 5)
    halo_blocks = [
        inverse(halo_volume[half], [sums[b][half] for b in range(5)]) for half in range(halves)
    ]
    halo_pre = precondition_halo(halo_residual)

    V, T, W, MIDDLE, SECOND, SUM = range(6)
    copy = finish_matrix(1, halo_pre)
    image = image_of(1, copy, pre)
    shadow = load_source()
    start_dots(0, [dot(shadow, shadow), dot(shadow, image)])
    save(V, image)
    pre = precondition(image)
    start_matrix(pre)
    halo_v = halo_image(2, halo_pre)
    halo_pre = precondition_halo(halo_v)

    copy = finish_matrix(2, halo_pre)
    twice = image_of(2, copy, pre)
    rho, shadow_image = wait_dots(0, 2)
    alpha = rho / shadow_image
    shadow, image = load_source(), load(V)
    middle = combine(shadow, -alpha, image)
    second = combine(image, -alpha, twice)
    start_dots(
        1, [dot(second, middle), dot(second, second), dot(shadow, middle), dot(shadow, second)]
    )
    save(T, twice)
    save(MIDDLE, middle)
    save(SECOND, second)
    pre = precondition(twice)
    start_matrix(pre)
    halo_t = halo_image(3, halo_pre)
    halo_pre = precondition_halo(halo_t)

    copy = finish_matrix(3, halo_pre)
    thrice = image_of(3, copy, pre)
    second_mid, second_sq, shadow_mid, shadow_second = wait_dots(1, 4)
    omega = second_mid / second_sq
    rho_next = shadow_mid - omega * shadow_second
    beta = rho_next / rho * (alpha / omega)
    shadow, image, twice, middle, second = (
        load_source(),
        load(V),
        load(T),
        load(MIDDLE),
        load(SECOND),
    )
    residual = combine(middle, -omega, second)
    image_residual = combine(second, -omega, combine(twice, -alpha, thrice))
    direction = combine(residual, beta, combine(shadow, -omega, image))
    next_image = combine(image_residual, beta, combine(image, -omega, twice))
    start_dots(2, [dot(shadow, next_image)])
    save(V, next_image)
    save(T, residual)
    save(W, image_residual)
    save(SUM, combine([alpha * x for x in shadow], omega, middle))
    save(MIDDLE, direction)
    pre = precondition(next_image)
    start_matrix(pre)
    halo_w = halo_image(4, halo_pre)
    halo_second = combine_halo(halo_v, -alpha, halo_t)
    halo_next = combine_halo(
        combine_halo(halo_second, -omega, combine_halo(halo_t, -alpha, halo_w)),
        beta,
        combine_halo(halo_v, -omega, halo_t),
    )
    copy = finish_matrix(4, precondition_halo(halo_next), last=True)
    (shadow_image,) = wait_dots(2, 1)
    alpha = rho_next / shadow_image
    middle = combine(load(T), -alpha, load(V))
    save(MIDDLE, combine(load(SUM), alpha, load(MIDDLE)))
    volume = volume_ref[...]
    base = combine(load(W), -alpha, [volume * v for v in pre])
    second = combine(base, -alpha, pair_sums(4, copy, 4))
    start_dots(3, [dot(second, middle), dot(second, second)])
    known = precondition(load(MIDDLE))
    pre_mid = precondition(middle)
    second_mid, second_sq = wait_dots(3, 2)
    omega = second_mid / second_sq
    for b in range(4):
        out_ref[pl.ds(b, tiles, stride=4), :] = known[b] + omega * pre_mid[b]
        out_ref[pl.ds(4 * tiles + b, tiles, stride=4), :] = middle[b] - omega * second[b]

    @pl.when(core == 0)
    def _():
        part = halo_in.at[0, 0]
        pltpu.make_async_copy(part, part, halo_send.at[0]).wait()
        for turn in range(dot_in.shape[0]):
            for part in (dot_in.at[turn, pl.ds(0, parts - 1)], dot_in.at[turn, pl.ds(0, parts)]):
                pltpu.make_async_copy(part, part, dot_send.at[turn]).wait()

    @pl.when(core == cores - 1)
    def _():
        part = halo_in.at[turns]
        pltpu.make_async_copy(part, part, halo_send.at[turns]).wait()

    for turn in range(1, turns):
        part = halo_part(turn)
        pltpu.make_async_copy(part, part, halo_send.at[turn]).wait()
    for copy in sent:
        copy.wait_send()


def body(
    flow_state,
    source_term,
    volume_rate,
    face_normal,
    face_owner,
    face_neighbour,
    face_count,
    send_list,
    halo_count,
):
    parts = lax.axis_size("cells")
    cores = lax.axis_size("faces")
    cells = flow_state.shape[1]
    tiles = cells // LANES
    pairs = tiles // 2
    groups = pairs // 8
    face_rows = face_owner.shape[0] // LANES
    lists, width = send_list.shape
    period = -(-(lists + 16) // 8) * 8
    turns = 1 + 2 * ITERS

    def by_tile(field):
        return field.reshape(4, tiles, LANES).transpose(1, 0, 2).reshape(4 * tiles, LANES)

    def by_component(field):
        return field.reshape(tiles, 4, LANES).transpose(1, 0, 2).reshape(4, cells)

    vmem = pl.BlockSpec(memory_space=pltpu.VMEM)
    hbm = pl.BlockSpec(memory_space=pltpu.HBM)
    ints = pltpu.VMEM((3, pairs, LANES), jnp.int32)
    floats = pltpu.VMEM((3, pairs, LANES), F32)
    hot = pltpu.VMEM((tiles, 3 * LANES // 2, 2 * LANES), BF16)
    both = pl.pallas_call(
        functools.partial(kernel, parts, cores),
        out_shape=pltpu.VMEM((8 * tiles, LANES), F32),
        in_specs=[hbm] * 9,
        out_specs=vmem,
        scratch_shapes=[
            pltpu.VMEM((4 * tiles, LANES), F32),
            pltpu.VMEM((4 * tiles, LANES), F32),
            pltpu.VMEM((tiles, LANES), F32),
            pltpu.VMEM((face_rows + 8, 3, LANES), F32),
            pltpu.VMEM((face_rows, LANES), jnp.int32),
            pltpu.VMEM((face_rows, LANES), jnp.int32),
            pltpu.VMEM((lists, width), jnp.int32),
            pltpu.SMEM((1,), jnp.int32),
            pltpu.SMEM((lists,), jnp.int32),
            pltpu.VMEM((8 * lists * width // LANES, LANES), jnp.int32),
            pltpu.VMEM((8 * lists * width // LANES, LANES), jnp.int32),
            pltpu.VMEM((40 * lists * width // LANES, LANES), F32),
            pltpu.SemaphoreType.DMA((9,)),
            ints,
            ints,
            ints,
            floats,
            floats,
            floats,
            floats,
            pltpu.VMEM((3, 3, pairs, LANES), F32),
            hot,
            pltpu.VMEM((pairs, 3 * LANES // 2, 2 * LANES), BF16),
            pltpu.VMEM((2, 3, 8 * pairs, LANES), F32),
            pltpu.VMEM((2, 3, 8 * pairs, LANES), F32),
            pltpu.VMEM((2, 8 * tiles + 8, LANES), F32),
            pltpu.VMEM((2, 8 * tiles + 8, LANES), F32),
            pltpu.VMEM((8 * tiles, LANES), F32),
            pltpu.VMEM((5 * tiles, LANES), F32),
            pltpu.VMEM((4, tiles + 8, LANES), F32),
            pltpu.VMEM((8 * period, LANES), F32),
            pltpu.VMEM((5, tiles, LANES), F32),
            pltpu.VMEM((6, 4, tiles, LANES), F32),
            pltpu.VMEM((turns, 5 * tiles + 16, LANES), F32),
            pltpu.VMEM((turns, 5 * tiles + 16, LANES), F32),
            pltpu.VMEM((turns + 1, lists, 16, LANES), F32),
            pltpu.VMEM((turns + 1, cores, 16 * lists, LANES), F32),
            pltpu.VMEM((turns + 8, 1, LANES), F32),
            pltpu.VMEM((turns - 1, parts + 8, 1, LANES), F32),
            pltpu.SemaphoreType.DMA((turns,)),
            pltpu.SemaphoreType.DMA((turns,)),
            pltpu.SemaphoreType.DMA((turns + 1,)),
            pltpu.SemaphoreType.DMA((turns + 1,)),
            pltpu.SemaphoreType.DMA((turns - 1,)),
            pltpu.SemaphoreType.DMA((turns - 1,)),
        ],
        compiler_params=pltpu.CompilerParams(
            collective_id=0, has_side_effects=True, vmem_limit_bytes=56 * 1024 * 1024
        ),
    )(
        face_count,
        by_tile(flow_state),
        by_tile(source_term),
        volume_rate.reshape(tiles, LANES),
        face_normal.reshape(3, face_rows, LANES).transpose(1, 0, 2),
        face_owner.reshape(face_rows, LANES),
        face_neighbour.reshape(face_rows, LANES),
        send_list,
        halo_count,
    )
    return by_component(both[: 4 * tiles]), by_component(both[4 * tiles :])


def solution(mesh):
    in_specs = (
        P(None, "cells"),
        P(None, "cells"),
        P("cells"),
        P(None, ("cells", "faces")),
        P(("cells", "faces")),
        P(("cells", "faces")),
        P(("cells", "faces")),
        P("cells", None),
        P("cells"),
    )
    out_specs = (P(None, "cells"), P(None, "cells"))
    return jax.shard_map(body, mesh=mesh, in_specs=in_specs, out_specs=out_specs, check_vma=False)
```

```python
import functools

import jax
import jax.numpy as jnp
from jax import lax
from jax.experimental import pallas as pl
from jax.experimental.pallas import tpu as pltpu
from jax.sharding import PartitionSpec as P

ITERS = 2
LANES = 128
MESH = pl.DeviceIdType.MESH
F32 = jnp.float32
BF16 = jnp.bfloat16


def take_lanes(source, index):
    return jnp.take_along_axis(source, index, axis=1, mode="promise_in_bounds")


def split(value):
    high = value.astype(BF16).astype(F32)
    rest = value - high
    middle = rest.astype(BF16).astype(F32)
    return high, middle, rest - middle


def woven(*queues):
    steps = [((i + 0.5) / len(q), n, f) for n, q in enumerate(queues) for i, f in enumerate(q)]
    for _, _, step in sorted(steps, key=lambda item: item[:2]):
        step()


def kernel(
    parts,
    cores,
    count_hbm,
    flow_hbm,
    source_hbm,
    volume_hbm,
    normal_hbm,
    owner_hbm,
    neighbour_hbm,
    list_hbm,
    halo_count_hbm,
    out_ref,
    flow_ref,
    source_ref,
    volume_ref,
    normal_ref,
    owner_ref,
    neighbour_ref,
    list_ref,
    count_ref,
    halo_count_ref,
    list_at,
    list_col,
    found_rows,
    input_sem,
    own_lane,
    right_lane,
    right_kind,
    own_row,
    local_row,
    face_u,
    face_s,
    face_n,
    signed_hot,
    own_hot,
    flux_rows,
    setup_rows,
    cell_rows,
    size_cells,
    own_cells,
    local_sums,
    fields,
    halo_rows,
    blocks,
    vecs,
    pair_out,
    pair_in,
    halo_out,
    halo_in,
    dot_out,
    dot_in,
    pair_send,
    pair_recv,
    halo_send,
    halo_recv,
    dot_send,
    dot_recv,
):
    me = lax.axis_index("cells")
    core = lax.axis_index("faces")
    other = (core + 1) % cores
    tiles = volume_ref.shape[0]
    pairs = tiles // 2
    groups = pairs // 8
    cells = tiles * LANES
    lists, width = list_ref.shape
    halves = width // LANES
    side = lists // 2
    lists_here = lists // cores
    period = halo_rows.shape[0] // (4 * halves)
    turns = pair_in.shape[0]
    offsets = [k + 1 if k < side else side - 1 - k for k in range(lists)]
    sooner = [k for k in range(lists) if offsets[k] % 2]
    later = [k for k in range(lists) if offsets[k] % 2 == 0]

    def fetched(number, source, target):
        copy = pltpu.make_async_copy(source, target, input_sem.at[number])
        copy.start()
        return copy

    first_copies = [
        fetched(7, halo_count_hbm, halo_count_ref),
        fetched(6, list_hbm, list_ref),
        fetched(2, flow_hbm, flow_ref),
        fetched(4, source_hbm, source_ref),
        fetched(5, volume_hbm, volume_ref),
    ]
    index_copies = [
        fetched(8, count_hbm, count_ref),
        fetched(0, owner_hbm, owner_ref),
        fetched(1, neighbour_hbm, neighbour_ref),
    ]
    normals = [fetched(3, normal_hbm, normal_ref.at[pl.ds(0, 3 * pairs)])]

    barrier = pltpu.get_barrier_semaphore()

    def signal_entry(cell, face):
        pl.semaphore_signal(
            barrier,
            inc=1,
            device_id={"cells": cell, "faces": face},
            device_id_type=MESH,
        )

    for place in range(1, parts):
        offset = (place + 1) // 2 if place % 2 else parts - place // 2
        cell = lax.rem(me + offset, parts)
        for c in range(cores):
            signal_entry(cell, c)
    for step in range(1, cores):
        signal_entry(me, lax.rem(core + step, cores))

    row8 = lax.broadcasted_iota(jnp.int32, (8, LANES), 0)

    def look_up(which, half, wanted, hs, first):
        number = len(wanted)
        at = pl.ds(8 * (halves * which + half), 8)
        row, col = list_at[at, :], list_col[at, :]
        masks = [row == row8 + 8 * h for h in hs]
        for b, field in enumerate(wanted):
            place = pl.ds(8 * (halves * number * which + number * half + b), 8)
            found = jnp.zeros((8, LANES), F32) if first else found_rows[place, :]
            for h, mask in zip(hs, masks):
                found = jnp.where(mask, take_lanes(field(h), col), found)
            found_rows[place, :] = found

    def row_sums(blocks_of):
        shift, level = 1, blocks_of
        while len(level) > 1:
            mask = (row8 // shift) % 2 == 0
            level = [
                jnp.where(mask, x, y) + pltpu.roll(jnp.where(mask, y, x), 8 - shift, 0)
                for x, y in zip(level[::2], level[1::2])
            ]
            shift *= 2
        return level[0]

    def listed(k, fills):
        number = len(fills)
        flat = [found_rows[pl.ds(8 * (halves * number * k + i), 8), :] for i in range(halves * number)]
        flat += [jnp.zeros((8, LANES), F32)] * (-len(flat) % 8)
        slot = lax.broadcasted_iota(jnp.int32, (8, LANES), 1)
        limit = halo_count_ref[k]
        tiles_of = []
        for first in range(0, len(flat), 8):
            row = row8 + first
            half = row // number
            used = slot + half * LANES < limit
            fill = jnp.zeros((8, LANES), F32)
            if fills[-1]:
                fill = jnp.where(row % number == number - 1, fills[-1], 0.0)
            tiles_of.append(jnp.where(used, row_sums(flat[first : first + 8]), fill))
        return tiles_of

    def send_halo(turn, rows, place, which):
        pitch = 8 if turn == 0 else 16
        for k in which:
            for c in range(cores):
                pltpu.make_async_remote_copy(
                    src_ref=halo_out.at[turn, k, pl.ds(0, rows)],
                    dst_ref=halo_in.at[turn, place, pl.ds(k * pitch, rows)],
                    send_sem=halo_send.at[turn],
                    recv_sem=halo_recv.at[turn],
                    device_id={"cells": lax.rem(me + offsets[k] + parts, parts), "faces": c},
                    device_id_type=MESH,
                ).start()

    def halo_part(turn):
        if turn == 0:
            return halo_in.at[turn, 0, pl.ds(0, 8 * lists)]
        return halo_in.at[turn] if turn == 1 else halo_in.at[turn, 0]

    def wait_halo(turn):
        part = halo_part(turn)
        pltpu.make_async_copy(part, part, halo_recv.at[turn]).wait()

    def halo_row(turn, place, row):
        pitch = 8 if turn == 0 else 16
        return halo_in[turn, place, pl.ds(row, lists, stride=pitch), :]

    def halo_sums(turn, number):
        return [
            [
                halo_row(turn, 0, half * number + b) + halo_row(turn, 1, half * number + b)
                for half in range(halves)
            ]
            for b in range(number)
        ]

    def look_up_all(turn, number, hs, first, which):
        def step(k, half):
            wanted = [functools.partial(partial_field, turn, b) for b in range(number)]
            return lambda: look_up(k, half, wanted, hs, first)

        return [step(k, half) for k in which for half in range(halves)]

    def put_listed(turn, fills, which):
        for k in which:
            for i, rows in enumerate(listed(k, fills)):
                halo_out[turn, k, pl.ds(8 * i, 8)] = rows
        return 8 * (-(-halves * len(fills) // 8))

    def pair_copy(turn, rows):
        part = pl.ds(0, rows)
        copy = pltpu.make_async_remote_copy(
            src_ref=pair_out.at[turn, part],
            dst_ref=pair_in.at[turn, part],
            send_sem=pair_send.at[turn],
            recv_sem=pair_recv.at[turn],
            device_id={"cells": me, "faces": other},
            device_id_type=MESH,
        )
        copy.start()
        return copy

    def start_dots(turn, partials):
        at = lax.broadcasted_iota(jnp.int32, (1, LANES), 1)
        packed = jnp.zeros((1, LANES), F32)
        for d, p in enumerate(partials):
            row = jnp.sum(p.reshape(tiles // 8, 8, LANES).sum(axis=0), axis=0, keepdims=True)
            packed = jnp.where(at == d, jnp.sum(row, axis=1, keepdims=True), packed)
        dot_out[turn] = packed

        @pl.when(core == 0)
        def _():
            dot_in[turn, me] = packed
            for place in range(1, parts):
                offset = (place + 1) // 2 if place % 2 else parts - place // 2
                for c in range(cores):
                    send_dots(turn, lax.rem(me + offset, parts), c)
            for c in range(1, cores):
                send_dots(turn, me, c)

    def send_dots(turn, cell, face):
        pltpu.make_async_remote_copy(
            src_ref=dot_out.at[turn],
            dst_ref=dot_in.at[turn, me],
            send_sem=dot_send.at[turn],
            recv_sem=dot_recv.at[turn],
            device_id={"cells": cell, "faces": face},
            device_id_type=MESH,
        ).start()

    def wait_dots(turn, number):
        @pl.when(core == 0)
        def _():
            part = dot_in.at[turn, pl.ds(0, parts - 1)]
            pltpu.make_async_copy(part, part, dot_recv.at[turn]).wait()

        @pl.when(core != 0)
        def _():
            part = dot_in.at[turn, pl.ds(0, parts)]
            pltpu.make_async_copy(part, part, dot_recv.at[turn]).wait()

        total = dot_in[turn, 0]
        for q in range(1, parts):
            total = total + dot_in[turn, q]
        return [jnp.broadcast_to(total[:, d : d + 1], (1, LANES)) for d in range(number)]

    def put_field(values):
        for b, value in enumerate(values):
            fields[b, pl.ds(0, tiles), :] = value
            fields[b, pl.ds(tiles, 1), :] = value[0:1]

    def put_halo(values):
        for b, value in enumerate(values):
            for half in range(halves):
                rows = jnp.concatenate([value[half]] * (-(-period // lists)), axis=0)
                halo_rows[pl.ds((halves * b + half) * period, period), :] = rows[:period]

    def by_tile(g, j, of_tile):
        if j == 0:
            return of_tile(0)
        if j == 2:
            return of_tile(1)
        early = lax.broadcasted_iota(jnp.int32, (8, LANES), 1) < LANES // 2
        return [jnp.where(early, x, y) for x, y in zip(of_tile(0), of_tile(1))]

    def local_sides(g, j, b):
        here = pl.ds(g * 8, 8)
        left_at = own_lane[j, here, :]
        right_at = right_lane[j, here, :]
        kind = right_kind[j, here, :]

        def of_tile(odd):
            first = 16 * g + odd
            low = fields[b, pl.ds(first, 8, stride=2), :]
            high = fields[b, pl.ds(first + 1, 8, stride=2), :]
            right = jnp.where(
                kind == 0,
                take_lanes(low, right_at),
                jnp.where(kind == 1, take_lanes(high, right_at), 0.0),
            )
            return [take_lanes(low, left_at), right]

        return by_tile(g, j, of_tile)

    def halo_side(g, j, b):
        here = pl.ds(g * 8, 8)
        right_at = right_lane[j, here, :]
        kind = right_kind[j, here, :]

        def of_tile(odd):
            first = (16 * g) % lists + odd
            low = halo_rows[pl.ds(2 * b * period + first, 8, stride=2), :]
            high = halo_rows[pl.ds((2 * b + 1) * period + first, 8, stride=2), :]
            right = jnp.where(
                kind == 2,
                take_lanes(low, right_at),
                jnp.where(kind == 3, take_lanes(high, right_at), 0.0),
            )
            return [right]

        return by_tile(g, j, of_tile)[0]

    def put_flux(ref, g, j, b, value):
        for part, piece in enumerate(split(value)):
            row = 4 * part + b if b < 4 else 12 + part
            ref[row // 8, j, pl.ds(64 * g + row % 8, 8, stride=8), :] = piece

    def tile_rows(rows_ref, u, odd):
        at = pl.ds(u * 8, 8)
        pieces = []
        for half in range(2):
            middle = rows_ref[half, 1, at, :]
            if odd:
                middle = pltpu.roll(middle, LANES // 2, 1)
            pieces.append(jnp.concatenate([rows_ref[half, 2 * odd, at, :], middle], axis=1))
        return jnp.concatenate(pieces, axis=0)[:, : 3 * LANES // 2].astype(BF16)

    def added(rows, hot):
        return lax.dot_general(
            rows, hot, (((1,), (0,)), ((), ())), preferred_element_type=F32
        )

    def put_cells(u, odd, low, high):
        at = u * 16 + odd * 8
        cell_rows[0, pl.ds(at, 8), :] = low
        cell_rows[1, pl.ds(at + 8, 8), :] = high

    def scatter(u):
        for odd in range(2):
            result = added(tile_rows(flux_rows, u, odd), signed_hot[2 * u + odd])
            result = result[:8] + result[8:]
            put_cells(u, odd, result[:, :LANES], result[:, LANES:])

    def own_sums(rows, u):
        result = added(jnp.concatenate(rows, axis=0), own_hot[u])
        return [result[16 * odd : 16 * odd + 16, odd * LANES : (odd + 1) * LANES] for odd in range(2)]

    def scatter_halo(u):
        rows = [tile_rows(flux_rows, u, odd) for odd in range(2)]
        for odd, result in enumerate(own_sums(rows, u)):
            own_cells[pl.ds(u * 16 + odd * 8, 8), :] = result[:8] + result[8:]

    def scatter_size(u):
        rows = [tile_rows(setup_rows, u, odd) for odd in range(2)]
        own = own_sums(rows, u)
        for odd in range(2):
            at = u * 16 + odd * 8
            result = added(rows[odd], signed_hot[2 * u + odd])
            low = lax.broadcasted_iota(jnp.int32, (8, 2 * LANES), 0) < 4
            summed = result[:8] + jnp.where(low, result[8:], 0.0)
            put_cells(u, odd, summed[:, :LANES], summed[:, LANES:])
            size_cells[0, pl.ds(at, 8), :] = 2.0 * own[odd][8:] - result[8:, :LANES]
            size_cells[1, pl.ds(at + 8, 8), :] = -result[8:, LANES:]

    def cell_sums(g, b):
        def rows(place, first):
            return cell_rows[place, pl.ds(first, 16, stride=8), :]

        first = 128 * g + b
        return rows(0, first) + rows(0, first + 4) + (rows(1, first) + rows(1, first + 4))

    def collect_local(g):
        for b in range(4):
            local_sums[pl.ds(tiles * b + 16 * g, 16), :] = cell_sums(g, b)
        if g == groups - 1:
            add_wraps(4)

    def add_wraps(number):
        for b in range(number):
            ref, places = (cell_rows, (b, b + 4)) if b < 4 else (size_cells, (4, 5, 6))
            wrap = [ref[1, pl.ds(8 * tiles + place, 1), :] for place in places]
            here = pl.ds(tiles * b, 8)
            wrap = jnp.where(row8 == 0, functools.reduce(jnp.add, wrap), 0.0)
            local_sums[here, :] = local_sums[here, :] + wrap

    def collect_halo(turn, g):
        for b in range(4):
            first = 128 * g + b
            here = pl.ds(tiles * b + 16 * g, 16)
            halo = own_cells[pl.ds(first, 16, stride=8), :]
            halo = halo + own_cells[pl.ds(first + 4, 16, stride=8), :]
            pair_out[turn, here, :] = local_sums[here, :] + halo

    def collect_setup(g):
        for b in range(4):
            local_sums[pl.ds(tiles * b + 16 * g, 16), :] = cell_sums(g, b)
        pieces = [
            size_cells[place, pl.ds(128 * g + row, 16, stride=8), :]
            for place in range(2)
            for row in (4, 5, 6)
        ]
        local_sums[pl.ds(4 * tiles + 16 * g, 16), :] = functools.reduce(jnp.add, pieces)
        if g == groups - 1:
            add_wraps(5)

    def collect_setup_halo(g):
        for b in range(5):
            here = pl.ds(tiles * b + 16 * g, 16)
            total = local_sums[here, :]
            if b in (0, 4):
                first = 128 * g + b // 4
                total = total + own_cells[pl.ds(first, 16, stride=8), :]
                total = total + own_cells[pl.ds(first + 4, 16, stride=8), :]
            pair_out[0, here, :] = total

    def partial_field(turn, b, h):
        return pair_out[turn, pl.ds(tiles * b + 8 * h, 8), :]

    def pair_sums(turn, copy, number):
        copy.wait_recv()
        parts_of = [pl.ds(tiles * b, tiles) for b in range(number)]
        return [pair_out[turn, rows, :] + pair_in[turn, rows, :] for rows in parts_of]

    sent = []

    def coefficients(g, j):
        here = pl.ds(g * 8, 8)
        n = [face_n[i, j, here, :] for i in range(3)]
        return face_u[j, here, :], face_s[j, here, :], n

    def put_fluxes(g, j, u, n, total, jump):
        for i in range(3):
            put_flux(flux_rows, g, j, i, u * total[i] + n[i] * total[3] - jump[i])
        last = n[0] * total[0] + n[1] * total[1] + n[2] * total[2] - jump[3]
        put_flux(flux_rows, g, j, 3, last)

    def local_steps(g):
        def step(j):
            u, s, n = coefficients(g, j)
            both = [local_sides(g, j, b) for b in range(4)]
            total = [left + right for left, right in both]
            jump = [s * (right - left) for left, right in both]
            put_fluxes(g, j, u, n, total, jump)

        return [functools.partial(step, j) for j in range(3)]

    def halo_steps(g):
        def step(j):
            u, s, n = coefficients(g, j)
            right = [halo_side(g, j, b) for b in range(4)]
            put_fluxes(g, j, u, n, right, [s * r for r in right])

        return [functools.partial(step, j) for j in range(3)]

    def over_groups(faces, spread, collect, turn=None, number=4):
        for stage in range(groups + 1 if turn is None else groups + 2):
            queues = []
            if stage < groups:
                queues.append(faces(stage))
            if 1 <= stage <= groups:
                first = 8 * (stage - 1)
                queues.append([functools.partial(spread, first + i) for i in range(8)])
            if turn is not None and stage >= 2:
                hs = [2 * (stage - 2), 2 * (stage - 2) + 1]
                queues.append(look_up_all(turn, number, hs, stage == 2, sooner))
            woven(*queues)
            if 1 <= stage <= groups:
                collect(stage - 1)

    def sent_sums(turn, number, last=False):
        fills = [0.0] * number
        if not last:
            rows = put_listed(turn + 1, fills, sooner)
            send_halo(turn + 1, rows, core, sooner)
        copy = pair_copy(turn, number * tiles)
        sent.append(copy)
        if not last:
            for step in look_up_all(turn, number, list(range(tiles // 8)), True, later):
                step()
            put_listed(turn + 1, fills, later)
            send_halo(turn + 1, rows, core, later)
        return copy

    def start_matrix(values):
        put_field(values)
        over_groups(local_steps, scatter, collect_local)

    def finish_matrix(turn, halos, last=False):
        put_halo(halos)
        collect = functools.partial(collect_halo, turn)
        over_groups(halo_steps, scatter_halo, collect, None if last else turn)
        return sent_sums(turn, 4, last)

    def image_of(turn, copy, values):
        sums = pair_sums(turn, copy, 4)
        volume = volume_ref[...]
        return [volume * values[b] + sums[b] for b in range(4)]

    def halo_image(turn, halos):
        wait_halo(turn)
        sums = halo_sums(turn, 4)
        return [
            [halo_volume[half] * halos[b][half] + sums[b][half] for half in range(halves)]
            for b in range(4)
        ]

    def solved(w, rvd, rschur, n):
        pressure = (w[3] - (n[0] * w[0] + n[1] * w[1] + n[2] * w[2]) * rvd) * rschur
        return [(w[i] - n[i] * pressure) * rvd for i in range(3)] + [pressure]

    def precondition(w):
        return solved(w, blocks[0], blocks[1], [blocks[2 + i] for i in range(3)])

    def precondition_halo(w):
        by_half = [
            solved([w[b][half] for b in range(4)], *halo_blocks[half]) for half in range(halves)
        ]
        return [[by_half[half][b] for half in range(halves)] for b in range(4)]

    def inverse(volume, sums):
        rvd = 1.0 / (volume + sums[0] + sums[4])
        n = sums[1:4]
        norm = n[0] * n[0] + n[1] * n[1] + n[2] * n[2]
        return rvd, 1.0 / (volume + sums[4] - norm * rvd), n

    def load(which):
        return [vecs[which, b] for b in range(4)]

    def save(which, values):
        for b in range(4):
            vecs[which, b] = values[b]

    def dot(a, b):
        return a[0] * b[0] + a[1] * b[1] + a[2] * b[2] + a[3] * b[3]

    def combine(a, scale, b):
        return [x + scale * y for x, y in zip(a, b)]

    def combine_halo(a, scale, b):
        return [[x + scale * y for x, y in zip(p, q)] for p, q in zip(a, b)]

    def load_source():
        return [source_ref[pl.ds(b, tiles, stride=4), :] for b in range(4)]

    def first_field(b, h):
        if b == 7:
            return volume_ref[pl.ds(8 * h, 8), :]
        ref, component = (flow_ref, b) if b < 3 else (source_ref, b - 3)
        return ref[pl.ds(32 * h + component, 8, stride=4), :]

    for copy in first_copies:
        copy.wait()
    for k in range(lists):
        for half in range(halves):
            cell = list_ref[k : k + 1, half * LANES : (half + 1) * LANES]
            cell = jnp.broadcast_to(cell, (8, LANES))
            at = pl.ds(8 * (halves * k + half), 8)
            list_at[at, :] = cell // LANES
            list_col[at, :] = cell - cell // LANES * LANES
    every = list(range(tiles // 8))
    every_list = list(range(lists))

    @pl.when(core == 0)
    def _():
        wanted = [functools.partial(first_field, b) for b in range(3)]
        for k in range(lists):
            for half in range(halves):
                look_up(k, half, wanted, every, True)
        put_listed(0, [0.0] * 3, every_list)

    @pl.when(core == cores - 1)
    def _():
        wanted = [functools.partial(first_field, b) for b in range(3, 8)]
        for k in range(lists):
            for half in range(halves):
                look_up(k, half, wanted, every, True)
        put_listed(turns, [0.0] * 4 + [1.0], every_list)

    pl.semaphore_wait(barrier, parts * cores - 1)

    @pl.when(core == 0)
    def _():
        send_halo(0, 8, 0, sooner + later)

    @pl.when(core == cores - 1)
    def _():
        send_halo(turns, 16, 0, sooner + later)

    lane = lax.broadcasted_iota(jnp.int32, (pairs, LANES), 1)
    pair_id = lax.broadcasted_iota(jnp.int32, (pairs, LANES), 0)
    late = lane >= LANES // 2
    for copy in index_copies:
        copy.wait()
    count = count_ref[0]
    for j in range(3):
        tile = 2 * pair_id + (0 if j == 0 else 1)
        if j == 1:
            tile = 2 * pair_id + late.astype(jnp.int32)
        owner = owner_ref[pl.ds(j, pairs, stride=3), :]
        beside = neighbour_ref[pl.ds(j, pairs, stride=3), :]
        live = (3 * pair_id + j) * LANES + lane < count
        is_local = beside < cells
        column = beside - tile * LANES
        column = jnp.where(column < 0, column + cells, column)
        slot = beside - cells - (tile % lists) * width
        place = jnp.where(is_local, column, slot)
        upper = place >= LANES
        own = owner - tile * LANES
        own_lane[j] = own
        right_lane[j] = jnp.where(upper, place - LANES, place)
        right_kind[j] = jnp.where(is_local, 0, 2) + upper.astype(jnp.int32)
        own_row[j] = jnp.where(live, own, -1).astype(F32)
        local_row[j] = jnp.where(live & is_local, column, -1).astype(F32)

    cell_id = lax.broadcasted_iota(jnp.int32, (LANES, LANES), 1).astype(F32).astype(BF16)
    one, zero = jnp.ones((), BF16), jnp.zeros((), BF16)

    def by_face(rows):
        flat = rows[...].reshape(3 * pairs, LANES)
        spare = -(3 * pairs) % LANES
        flat = jnp.concatenate([flat, jnp.zeros((spare, LANES), F32)], axis=0)
        return flat.T.astype(BF16)

    own_faces, local_faces = by_face(own_row), by_face(local_row)

    def hot_of(column):
        return jnp.where(cell_id == column, one, zero)

    for u in range(pairs):
        for j in range(3):
            at = j * pairs + u
            own = jnp.broadcast_to(own_faces[:, at : at + 1], (LANES, LANES))
            local = jnp.broadcast_to(local_faces[:, at : at + 1], (LANES, LANES))
            own_cell = hot_of(own)
            low = own_cell - hot_of(local)
            high = -hot_of(local - LANES)
            half = LANES // 2
            if j == 1:
                places = [(2 * u, LANES, 0, half), (2 * u + 1, LANES, half, LANES)]
            else:
                places = [(2 * u + j // 2, 0, 0, LANES)]
            for tile, row, first, last in places:
                rows = slice(row, row + last - first)
                signed_hot[tile, rows, :LANES] = low[first:last]
                signed_hot[tile, rows, LANES:] = high[first:last]
                lanes = slice(tile % 2 * LANES, (tile % 2 + 1) * LANES)
                own_hot[u, rows, lanes] = own_cell[first:last]

    setup_rows[...] = jnp.zeros_like(setup_rows)
    flux_rows[...] = jnp.zeros_like(flux_rows)
    cell_rows[1, :8, :] = jnp.zeros((8, LANES), F32)
    size_cells[1, :8, :] = jnp.zeros((8, LANES), F32)
    for copy in normals:
        copy.wait()

    put_field([flow_ref[pl.ds(b, tiles, stride=4), :] for b in range(3)])
    def face_steps(g):
        def step(j):
            here = pl.ds(g * 8, 8)
            inside = right_kind[j, here, :] < 2
            n = [normal_ref[pl.ds(24 * g + j, 8, stride=3), i, :] for i in range(3)]
            both = [local_sides(g, j, b) for b in range(3)]
            total = [left + right for left, right in both]
            u = 0.25 * (n[0] * total[0] + n[1] * total[1] + n[2] * total[2])
            size = jnp.sqrt(n[0] * n[0] + n[1] * n[1] + n[2] * n[2])
            face_u[j, here, :] = u
            face_s[j, here, :] = size
            put_flux(setup_rows, g, j, 0, jnp.where(inside, u, 0.0))
            for i in range(3):
                half = 0.5 * n[i]
                face_n[i, j, here, :] = half
                put_flux(setup_rows, g, j, 1 + i, half)
            put_flux(setup_rows, g, j, 4, jnp.where(inside, jnp.abs(u) + size, 0.0))

        return [functools.partial(step, j) for j in range(3)]

    def face_halo_steps(g):
        def step(j):
            here = pl.ds(g * 8, 8)
            outside = right_kind[j, here, :] >= 2
            u, size, n = coefficients(g, j)
            right = [halo_side(g, j, b) for b in range(3)]
            u = u + 0.5 * (n[0] * right[0] + n[1] * right[1] + n[2] * right[2])
            s = jnp.abs(u) + size
            face_u[j, here, :] = u
            face_s[j, here, :] = s
            put_flux(flux_rows, g, j, 0, jnp.where(outside, u, 0.0))
            put_flux(flux_rows, g, j, 1, jnp.where(outside, s, 0.0))

        return [functools.partial(step, j) for j in range(3)]

    over_groups(face_steps, scatter_size, collect_setup)
    wait_halo(0)
    put_halo([[halo_row(0, 0, half * 3 + b) for half in range(halves)] for b in range(3)])

    over_groups(face_halo_steps, scatter_halo, collect_setup_halo, 0, 5)
    copy = sent_sums(0, 5)
    rvd, rschur, coupling = inverse(volume_ref[...], pair_sums(0, copy, 5))
    blocks[0] = rvd
    blocks[1] = rschur
    for i in range(3):
        blocks[2 + i] = coupling[i]

    shadow = load_source()
    pre = precondition(shadow)
    start_matrix(pre)
    wait_halo(turns)

    def first_halo(b):
        return [halo_row(turns, 0, half * 5 + b) for half in range(halves)]

    halo_volume = first_halo(4)
    halo_residual = [first_halo(b) for b in range(4)]
    wait_halo(1)
    sums = halo_sums(1, 5)
    halo_blocks = [
        inverse(halo_volume[half], [sums[b][half] for b in range(5)]) for half in range(halves)
    ]
    halo_pre = precondition_halo(halo_residual)

    V, T, W, MIDDLE, SECOND, SUM = range(6)
    copy = finish_matrix(1, halo_pre)
    image = image_of(1, copy, pre)
    shadow = load_source()
    start_dots(0, [dot(shadow, shadow), dot(shadow, image)])
    save(V, image)
    pre = precondition(image)
    start_matrix(pre)
    halo_v = halo_image(2, halo_pre)
    halo_pre = precondition_halo(halo_v)

    copy = finish_matrix(2, halo_pre)
    twice = image_of(2, copy, pre)
    rho, shadow_image = wait_dots(0, 2)
    alpha = rho / shadow_image
    shadow, image = load_source(), load(V)
    middle = combine(shadow, -alpha, image)
    second = combine(image, -alpha, twice)
    start_dots(
        1, [dot(second, middle), dot(second, second), dot(shadow, middle), dot(shadow, second)]
    )
    save(T, twice)
    save(MIDDLE, middle)
    save(SECOND, second)
    pre = precondition(twice)
    start_matrix(pre)
    halo_t = halo_image(3, halo_pre)
    halo_pre = precondition_halo(halo_t)

    copy = finish_matrix(3, halo_pre)
    thrice = image_of(3, copy, pre)
    second_mid, second_sq, shadow_mid, shadow_second = wait_dots(1, 4)
    omega = second_mid / second_sq
    rho_next = shadow_mid - omega * shadow_second
    beta = rho_next / rho * (alpha / omega)
    shadow, image, twice, middle, second = (
        load_source(),
        load(V),
        load(T),
        load(MIDDLE),
        load(SECOND),
    )
    residual = combine(middle, -omega, second)
    image_residual = combine(second, -omega, combine(twice, -alpha, thrice))
    direction = combine(residual, beta, combine(shadow, -omega, image))
    next_image = combine(image_residual, beta, combine(image, -omega, twice))
    start_dots(2, [dot(shadow, next_image)])
    save(V, next_image)
    save(T, residual)
    save(W, image_residual)
    save(SUM, combine([alpha * x for x in shadow], omega, middle))
    save(MIDDLE, direction)
    pre = precondition(next_image)
    start_matrix(pre)
    halo_w = halo_image(4, halo_pre)
    halo_second = combine_halo(halo_v, -alpha, halo_t)
    halo_next = combine_halo(
        combine_halo(halo_second, -omega, combine_halo(halo_t, -alpha, halo_w)),
        beta,
        combine_halo(halo_v, -omega, halo_t),
    )
    copy = finish_matrix(4, precondition_halo(halo_next), last=True)
    (shadow_image,) = wait_dots(2, 1)
    alpha = rho_next / shadow_image
    middle = combine(load(T), -alpha, load(V))
    save(MIDDLE, combine(load(SUM), alpha, load(MIDDLE)))
    volume = volume_ref[...]
    base = combine(load(W), -alpha, [volume * v for v in pre])
    second = combine(base, -alpha, pair_sums(4, copy, 4))
    start_dots(3, [dot(second, middle), dot(second, second)])
    known = precondition(load(MIDDLE))
    pre_mid = precondition(middle)
    second_mid, second_sq = wait_dots(3, 2)
    omega = second_mid / second_sq
    for b in range(4):
        out_ref[pl.ds(b, tiles, stride=4), :] = known[b] + omega * pre_mid[b]
        out_ref[pl.ds(4 * tiles + b, tiles, stride=4), :] = middle[b] - omega * second[b]

    @pl.when(core == 0)
    def _():
        part = halo_in.at[0, 0]
        pltpu.make_async_copy(part, part, halo_send.at[0]).wait()
        for turn in range(dot_in.shape[0]):
            for part in (dot_in.at[turn, pl.ds(0, parts - 1)], dot_in.at[turn, pl.ds(0, parts)]):
                pltpu.make_async_copy(part, part, dot_send.at[turn]).wait()

    @pl.when(core == cores - 1)
    def _():
        part = halo_in.at[turns]
        pltpu.make_async_copy(part, part, halo_send.at[turns]).wait()

    for turn in range(1, turns):
        part = halo_part(turn)
        pltpu.make_async_copy(part, part, halo_send.at[turn]).wait()
    for copy in sent:
        copy.wait_send()


def body(
    flow_state,
    source_term,
    volume_rate,
    face_normal,
    face_owner,
    face_neighbour,
    face_count,
    send_list,
    halo_count,
):
    parts = lax.axis_size("cells")
    cores = lax.axis_size("faces")
    cells = flow_state.shape[1]
    tiles = cells // LANES
    pairs = tiles // 2
    groups = pairs // 8
    face_rows = face_owner.shape[0] // LANES
    lists, width = send_list.shape
    period = -(-(lists + 16) // 8) * 8
    turns = 1 + 2 * ITERS

    def by_tile(field):
        return field.reshape(4, tiles, LANES).transpose(1, 0, 2).reshape(4 * tiles, LANES)

    def by_component(field):
        return field.reshape(tiles, 4, LANES).transpose(1, 0, 2).reshape(4, cells)

    vmem = pl.BlockSpec(memory_space=pltpu.VMEM)
    hbm = pl.BlockSpec(memory_space=pltpu.HBM)
    ints = pltpu.VMEM((3, pairs, LANES), jnp.int32)
    floats = pltpu.VMEM((3, pairs, LANES), F32)
    hot = pltpu.VMEM((tiles, 3 * LANES // 2, 2 * LANES), BF16)
    both = pl.pallas_call(
        functools.partial(kernel, parts, cores),
        out_shape=pltpu.VMEM((8 * tiles, LANES), F32),
        in_specs=[hbm] * 9,
        out_specs=vmem,
        scratch_shapes=[
            pltpu.VMEM((4 * tiles, LANES), F32),
            pltpu.VMEM((4 * tiles, LANES), F32),
            pltpu.VMEM((tiles, LANES), F32),
            pltpu.VMEM((face_rows + 8, 3, LANES), F32),
            pltpu.VMEM((face_rows, LANES), jnp.int32),
            pltpu.VMEM((face_rows, LANES), jnp.int32),
            pltpu.VMEM((lists, width), jnp.int32),
            pltpu.SMEM((1,), jnp.int32),
            pltpu.SMEM((lists,), jnp.int32),
            pltpu.VMEM((8 * lists * width // LANES, LANES), jnp.int32),
            pltpu.VMEM((8 * lists * width // LANES, LANES), jnp.int32),
            pltpu.VMEM((40 * lists * width // LANES, LANES), F32),
            pltpu.SemaphoreType.DMA((9,)),
            ints,
            ints,
            ints,
            floats,
            floats,
            floats,
            floats,
            pltpu.VMEM((3, 3, pairs, LANES), F32),
            hot,
            pltpu.VMEM((pairs, 3 * LANES // 2, 2 * LANES), BF16),
            pltpu.VMEM((2, 3, 8 * pairs, LANES), F32),
            pltpu.VMEM((2, 3, 8 * pairs, LANES), F32),
            pltpu.VMEM((2, 8 * tiles + 8, LANES), F32),
            pltpu.VMEM((2, 8 * tiles + 8, LANES), F32),
            pltpu.VMEM((8 * tiles, LANES), F32),
            pltpu.VMEM((5 * tiles, LANES), F32),
            pltpu.VMEM((4, tiles + 8, LANES), F32),
            pltpu.VMEM((8 * period, LANES), F32),
            pltpu.VMEM((5, tiles, LANES), F32),
            pltpu.VMEM((6, 4, tiles, LANES), F32),
            pltpu.VMEM((turns, 5 * tiles, LANES), F32),
            pltpu.VMEM((turns, 5 * tiles, LANES), F32),
            pltpu.VMEM((turns + 1, lists, 16, LANES), F32),
            pltpu.VMEM((turns + 1, cores, 16 * lists, LANES), F32),
            pltpu.VMEM((turns + 8, 1, LANES), F32),
            pltpu.VMEM((turns - 1, parts + 8, 1, LANES), F32),
            pltpu.SemaphoreType.DMA((turns,)),
            pltpu.SemaphoreType.DMA((turns,)),
            pltpu.SemaphoreType.DMA((turns + 1,)),
            pltpu.SemaphoreType.DMA((turns + 1,)),
            pltpu.SemaphoreType.DMA((turns - 1,)),
            pltpu.SemaphoreType.DMA((turns - 1,)),
        ],
        compiler_params=pltpu.CompilerParams(
            collective_id=0, has_side_effects=True, vmem_limit_bytes=56 * 1024 * 1024
        ),
    )(
        face_count,
        by_tile(flow_state),
        by_tile(source_term),
        volume_rate.reshape(tiles, LANES),
        face_normal.reshape(3, face_rows, LANES).transpose(1, 0, 2),
        face_owner.reshape(face_rows, LANES),
        face_neighbour.reshape(face_rows, LANES),
        send_list,
        halo_count,
    )
    return by_component(both[: 4 * tiles]), by_component(both[4 * tiles :])


def solution(mesh):
    in_specs = (
        P(None, "cells"),
        P(None, "cells"),
        P("cells"),
        P(None, ("cells", "faces")),
        P(("cells", "faces")),
        P(("cells", "faces")),
        P(("cells", "faces")),
        P("cells", None),
        P("cells"),
    )
    out_specs = (P(None, "cells"), P(None, "cells"))
    return jax.shard_map(body, mesh=mesh, in_specs=in_specs, out_specs=out_specs, check_vma=False)
```
